32 devices in a mesh: snap: 4 (over z), param: 8 (over y, x, core).
Axes of the slice: x: 2, y: 2, z: 4, core: 2. Of those that a mesh axis runs over, the one named last changes fastest.
Arguments:
- snapshots: bfloat16 [256, 512, 1024], P('snap', 'param'), as said below
- coeffs: float32 [16, 256], P(None, 'snap'), may hold values from -0.375 to 0.375
Outputs:
- averages: float32 [16, 512, 1024], P(None, 'param', 'snap')
- width_norms: float32 [16], replicated
The draws below stay inside these ranges and needn't reach their ends.
Inputs may be any that keep to these rules, and one draw needn't show every extreme that they name: `snapshots`: stored snapshot weights, finite.
All inputs are finite; a program needn't handle non-finite values.
Results may differ from the reference program's by a relative error of at most 0.0003.
Values may be sent and summed in bfloat16 or wider, within the bound.
A program may use at most 64 MiB of HBM per device.

```python
import math
import jax
import jax.numpy as jnp
from jax import lax

WIDTHS = 16
COLS = 1024
NSNAP = 256
ROWS = 512


def draw_snapshots(key, part):
    key_rows = jax.random.fold_in(key, 11)
    key_cols = jax.random.fold_in(key, 12)
    key_base = jax.random.fold_in(key, 13)
    row_index = jnp.arange(ROWS, dtype=jnp.float32)
    row_scale = 3.0 ** (row_index / ROWS) * 10.0 ** jax.random.uniform(key_rows, (ROWS,), jnp.float32)
    col_scale = 10.0 ** jax.random.uniform(key_cols, (COLS,), jnp.float32)
    base = jax.random.normal(key_base, (NSNAP, ROWS, COLS), jnp.float32)
    values = base * row_scale[None, :, None] * col_scale[None, None, :] / 10.0
    return values.astype(jnp.bfloat16)


def block_scale(key, shape, shards, least, largest):
    loudness, own = 1.0, jax.random.fold_in(key, 6)
    for dim, blocks in shards:
        draws = jnp.exp(jax.random.uniform(jax.random.fold_in(own, dim), (blocks,), jnp.float32, least / len(shards), largest / len(shards)))
        loudness = loudness * jnp.repeat(draws, shape[dim] // blocks).reshape([-1 if axis == dim else 1 for axis in range(len(shape))])
    return loudness


def gaussian(rng, extent, deviation, most, cuts=(), kind=jnp.bfloat16):
    values = jax.random.normal(rng, extent, jnp.float32) * deviation
    if len(cuts) > 0:
        values = block_scale(rng, extent, cuts, -0.22, 0.18) * values
    return jnp.clip(values, min=-most, max=most).astype(kind)


def setup_inputs(seed: int = 0) -> dict:
    splits = jax.random.split(jax.random.key(seed), 3)
    snapshots = draw_snapshots(jax.random.fold_in(splits[2], 71), 0)
    coeffs = gaussian(splits[1], (WIDTHS, NSNAP), NSNAP ** -0.5, 0.375, ((1, 4),), jnp.float32)
    return dict(snapshots=snapshots, coeffs=coeffs)


def reference(snapshots, coeffs):
    block_rows = math.gcd(ROWS, 256)
    block_count = ROWS // block_rows

    def one_block(block_index):
        start = (block_index * block_rows).astype(jnp.int32)
        piece = lax.dynamic_slice_in_dim(snapshots, start, block_rows, 1).astype(jnp.float32)
        flat = piece.reshape(NSNAP, block_rows * COLS)
        product = jnp.dot(coeffs.astype(jnp.float32), flat, precision=lax.Precision.HIGHEST, preferred_element_type=jnp.float32)
        return product.reshape(WIDTHS, block_rows, COLS)
    stacked = lax.map(one_block, jnp.arange(block_count, dtype=jnp.int32))
    averages = jnp.transpose(stacked, (1, 0, 2, 3)).reshape(WIDTHS, ROWS, COLS)
    squares = lax.optimization_barrier(jnp.sum(averages * averages, axis=(1, 2)))
    width_norms = jnp.sqrt(squares / jnp.float32(ROWS * COLS))
    return (averages, width_norms)
```

```python
import functools

import jax
import jax.numpy as jnp
from jax import lax
from jax.experimental import pallas as pl
from jax.experimental.pallas import tpu as pltpu
from jax.sharding import PartitionSpec as P

MESH = pl.DeviceIdType.MESH
GROUP = 16
WIDE = 128
LAG = 3
LATE = 5
POWER = 15
AHEAD = 6
TOP = 2.0**8.375


def encode(value):
    largest = jnp.max(jnp.max(jnp.abs(value), axis=0), axis=0, keepdims=True)
    largest = jnp.maximum(largest, 1e-30)
    x = value * (TOP / largest)[None]
    x2 = x * x
    x4 = x2 * x2
    x8 = x4 * x4
    return ((x8 * x4) * (x2 * x)).astype(jnp.bfloat16), largest * (1.0 / TOP)


def decode(code, scale):
    y = code.astype(jnp.float32)
    size = jnp.exp2(jnp.log2(jnp.maximum(jnp.abs(y), 1e-38)) * (1.0 / POWER)) * scale[None]
    return jnp.where(y > 0.0, size, jnp.where(y < 0.0, -size, 0.0))


def each(size, body):
    if size <= 8:
        for k in range(size):
            body(k)
    else:
        pl.loop(0, size)(body)


def kernel(
    n, peers, entries, coeffs, stored, averages, norms,
    weights, spread, tiles, part, out_code, out_scale, in_code, in_scale, squares, lines,
    coeff_sem, load_sem, send_sem, send_scale_sem, recv_sem, recv_scale_sem,
    line_send, line_recv, known, token_up, token_down, complete,
):
    z = lax.axis_index("snap")
    me = lax.axis_index("param")
    widths, count = coeffs.shape
    keep = stored.shape[2] // n
    cuts = keep // WIDE
    groups = stored.shape[1] // GROUP * cuts
    steps = (n - 1) * groups
    lag = min(LAG, groups - 1)
    late = max(0, min(LATE, groups - lag, (n - 3) * (groups - lag)))
    low = z < n // 2
    first, final = z == 0, z == n - 1
    end = jnp.logical_or(first, final)
    middle = jnp.logical_not(end)
    hub = middle if n > 2 else end

    def turned(d, s, last):
        return jnp.where(d == last, groups - 1 - s, s) if late > 0 else s

    def upwards(k):
        d = n - 1 - k // groups
        return d, turned(d, lax.rem(k, groups), n - 2)

    def downwards(k):
        d = k // groups
        return d, turned(d, lax.rem(k, groups), 1)

    def own(i):
        du, tu = upwards(i)
        dd, td = downwards(i)
        return jnp.where(low, du, dd), jnp.where(low, tu, td)

    def spot(t):
        return (
            pl.ds(pl.multiple_of(t // cuts * GROUP, GROUP), GROUP),
            pl.ds(pl.multiple_of(lax.rem(t, cuts) * WIDE, WIDE), WIDE),
        )

    def load(i):
        d, t = own(i)
        column = d * keep + lax.rem(t, cuts) * WIDE
        return pltpu.make_async_copy(
            stored.at[:, pl.ds(pl.multiple_of(t // cuts * GROUP, GROUP), GROUP), pl.ds(pl.multiple_of(column, WIDE), WIDE)],
            tiles.at[i],
            load_sem.at[i],
        )

    read = pltpu.make_async_copy(coeffs, weights, coeff_sem)
    read.start()
    load(0).start()
    barrier = pltpu.get_barrier_semaphore()

    @pl.when(z > 0)
    def _():
        pl.semaphore_signal(barrier, inc=1, device_id={"snap": z - 1}, device_id_type=MESH)

    @pl.when(z < n - 1)
    def _():
        pl.semaphore_signal(barrier, inc=1, device_id={"snap": z + 1}, device_id_type=MESH)

    for i in range(1, min(AHEAD, n * groups)):
        load(i).start()

    def to_peers(semaphore):
        def body(k):
            @pl.when(k != me)
            def _():
                pl.semaphore_signal(semaphore, inc=1, device_id={"param": k}, device_id_type=MESH)

        each(peers, body)

    @pl.when(hub)
    def _():
        to_peers(barrier)

    tall, wide = spread.shape
    row = lax.broadcasted_iota(jnp.int32, (count, wide), 0)
    col = lax.broadcasted_iota(jnp.int32, (count, wide), 1)
    repeat = jnp.where(col // GROUP == row, 1.0, 0.0).astype(jnp.bfloat16)
    row = lax.broadcasted_iota(jnp.int32, (GROUP, wide), 0)
    col = lax.broadcasted_iota(jnp.int32, (GROUP, wide), 1)
    same = (row == col % GROUP)[None]
    read.wait()
    whole = weights[...]
    high = whole.astype(jnp.bfloat16)
    rest = (whole - high.astype(jnp.float32)).astype(jnp.bfloat16)
    both = jnp.concatenate([high, rest], axis=0)
    full = jnp.dot(both, repeat, preferred_element_type=jnp.float32)
    full = jnp.where(same, full[:, None, :], 0.0)
    spread[...] = full.reshape(tall, wide).astype(jnp.bfloat16)
    squares[...] = jnp.zeros_like(squares)

    def copies(way, k, peer):
        code = pltpu.make_async_remote_copy(
            src_ref=out_code.at[way, k], dst_ref=in_code.at[way, k],
            send_sem=send_sem.at[way, k], recv_sem=recv_sem.at[way, k],
            device_id={"snap": peer}, device_id_type=MESH,
        )
        scale = pltpu.make_async_remote_copy(
            src_ref=out_scale.at[way, k], dst_ref=in_scale.at[way, k],
            send_sem=send_scale_sem.at[way, k], recv_sem=recv_scale_sem.at[way, k],
            device_id={"snap": peer}, device_id_type=MESH,
        )
        return scale, code

    def send(way, k, peer, value):
        code, scale = encode(value)
        out_code[way, k] = code
        out_scale[way, k] = scale
        for copy in copies(way, k, peer):
            copy.start()

    def arrived(way, k):
        for copy in copies(way, k, jnp.where(z == n - 1, z - 1, z + 1)):
            copy.wait_recv()
        return decode(in_code[way, k], in_scale[way, k])

    def count_squares(value):
        squares[...] += jnp.sum((value * value).reshape(widths, GROUP // 8, 8, WIDE), axis=1)

    half = widths * GROUP
    total = n * groups

    @pl.loop(0, total)
    def _(i):
        d, t = own(i)
        load(i).wait()

        @pl.when(i + AHEAD < total)
        def _():
            load(i + AHEAD).start()

        both_parts = jnp.dot(
            spread[...], tiles[i].reshape(count * GROUP, WIDE), preferred_element_type=jnp.float32
        )
        value = (both_parts[:half] + both_parts[half:]).reshape(widths, GROUP, WIDE)
        part[d, t] = value

        @pl.when(jnp.logical_and(i == 0, end))
        def _():
            pl.semaphore_wait(barrier, 1 if n > 2 else peers)

        @pl.when(jnp.logical_and(end, d != z))
        def _():
            send(jnp.where(first, 0, 1), i, jnp.where(first, 1, n - 2), value)

        @pl.when(jnp.logical_and(i == total // 4, middle))
        def _():
            pl.semaphore_wait(barrier, 2 + peers - 1)

        @pl.when(jnp.logical_and(i == total // 4, hub))
        def _():
            to_peers(known)

        @pl.when(jnp.logical_and(i == total // 2, hub))
        def _():
            pl.semaphore_wait(known, peers - 1)

        @pl.when(jnp.logical_and(i == total // 2, middle))
        def _():
            @pl.when(z > 1)
            def _():
                pl.semaphore_signal(token_down, inc=1, device_id={"snap": z - 1}, device_id_type=MESH)

            @pl.when(z < n - 2)
            def _():
                pl.semaphore_signal(token_up, inc=1, device_id={"snap": z + 1}, device_id_type=MESH)

    if n > 4:
        raise NotImplementedError

    @pl.when(middle)
    def _():
        @pl.when(z > 1)
        def _():
            pl.semaphore_wait(token_up, 1)

        @pl.when(z < n - 2)
        def _():
            pl.semaphore_wait(token_down, 1)

        @pl.when(z == 1)
        def _():
            pl.semaphore_signal(complete, inc=1, device_id={"snap": z - 1}, device_id_type=MESH)

        @pl.when(z == n - 2)
        def _():
            pl.semaphore_signal(complete, inc=1, device_id={"snap": z + 1}, device_id_type=MESH)

    def settle(t, value, counted):
        rows, columns = spot(t)
        averages[:, rows, columns] = value

        @pl.when(counted)
        def _():
            count_squares(value)

    def pass_on(j):
        up = j - lag * (z - 1)
        down = j - lag * (n - 2 - z)

        @pl.when(jnp.logical_and(up >= 0, up < (n - z) * groups))
        def _():
            d, t = upwards(up)
            value = part[d, t] + arrived(0, up)

            @pl.when(d == z)
            def _():
                s = jnp.where(z == 1, groups - 1 - t, t) if late > 0 else t
                second = z * groups + s + lag * (n - 2 - z) < j

                @pl.when(second)
                def _():
                    settle(t, value, jnp.logical_or(z != 1, t < groups - late))

                @pl.when(jnp.logical_not(second))
                def _():
                    part[d, t] = value

            extra = jnp.logical_and(z == n - 2, up < groups + late) if late > 0 else False

            @pl.when(jnp.logical_or(d != z, extra))
            def _():
                send(0, up, z + 1, value)

        @pl.when(jnp.logical_and(down >= 0, down < (z + 1) * groups))
        def _():
            d, t = downwards(down)
            value = part[d, t] + arrived(1, down)

            @pl.when(d == z)
            def _():
                s = jnp.where(z == n - 2, groups - 1 - t, t) if late > 0 else t
                second = (n - 1 - z) * groups + s + lag * (z - 1) <= j

                @pl.when(second)
                def _():
                    settle(t, value, jnp.logical_or(z != n - 2, t < groups - late))

                @pl.when(jnp.logical_not(second))
                def _():
                    part[d, t] = value

            extra = jnp.logical_and(z == 1, down < groups + late) if late > 0 else False

            @pl.when(jnp.logical_or(d != z, extra))
            def _():
                send(1, down, z - 1, value)

    @pl.when(middle)
    def _():
        pl.loop(0, steps - late)(pass_on)

    @pl.when(end)
    def _():
        @pl.loop(0, groups + late)
        def _(k):
            way = jnp.where(first, 1, 0)
            t = jnp.where(k < groups, k, 2 * groups - 1 - k)
            d = jnp.where(k < groups, z, jnp.where(first, 1, n - 2))
            value = part[d, t] + arrived(way, k)
            count_squares(value)

            @pl.when(k < groups)
            def _():
                rows, columns = spot(t)
                averages[:, rows, columns] = value

        if n > 2:
            pl.semaphore_wait(complete, 1)

    sums = jnp.sum(jnp.sum(squares[...], axis=1), axis=1, keepdims=True)
    lanes = norms.shape[1]
    row = lax.broadcasted_iota(jnp.int32, (widths, lanes), 0)
    col = lax.broadcasted_iota(jnp.int32, (widths, lanes), 1)
    line = jnp.sum(jnp.where(row == col, sums, 0.0), axis=0, keepdims=True)

    mine = z * peers + me
    lines[mine] = line

    def others(act):
        for p in range(n):
            def body(k, p=p):
                @pl.when(jnp.logical_or(p != z, k != me))
                def _():
                    act(p, k)

            each(peers, body)

    def line_copy(p, k, slot):
        return pltpu.make_async_remote_copy(
            src_ref=lines.at[slot], dst_ref=lines.at[slot],
            send_sem=line_send.at[p * peers + k], recv_sem=line_recv.at[slot],
            device_id={"snap": p, "param": k}, device_id_type=MESH,
        )

    others(lambda p, k: line_copy(p, k, mine).start())

    if late > 0:
        @pl.when(middle)
        def _():
            pl.loop(steps - late, steps)(pass_on)

    up_sends = (n - 1 - z) * groups
    down_sends = z * groups
    if late > 0:
        up_sends += jnp.where(z == n - 2, late, 0)
        down_sends += jnp.where(z == 1, late, 0)

    @pl.loop(0, steps)
    def _(k):
        @pl.when(k < up_sends)
        def _():
            for copy in copies(0, k, jnp.where(final, z - 1, z + 1)):
                copy.wait_send()

        @pl.when(k < down_sends)
        def _():
            for copy in copies(1, k, jnp.where(first, z + 1, z - 1)):
                copy.wait_send()

    others(lambda p, k: line_copy(p, k, mine).wait_send())
    others(lambda p, k: line_copy(p, k, p * peers + k).wait_recv())
    norms[...] = jnp.sqrt(jnp.sum(lines[...], axis=0) / jnp.float32(entries))


def on_device(n, peers, snapshots, coeffs):
    count, height, cols = snapshots.shape
    widths = coeffs.shape[0]
    keep = cols // n
    groups = height // GROUP * (keep // WIDE)
    steps = (n - 1) * groups
    entries = height * cols * peers
    dma = pltpu.SemaphoreType.DMA
    regular = pltpu.SemaphoreType.REGULAR
    averages, norms = pl.pallas_call(
        functools.partial(kernel, n, peers, entries),
        out_shape=(
            jax.ShapeDtypeStruct((widths, height, keep), jnp.float32),
            jax.ShapeDtypeStruct((1, 128), jnp.float32),
        ),
        in_specs=[pl.BlockSpec(memory_space=pltpu.HBM), pl.BlockSpec(memory_space=pl.ANY)],
        out_specs=(pl.BlockSpec(memory_space=pltpu.VMEM), pl.BlockSpec(memory_space=pltpu.VMEM)),
        scratch_shapes=[
            pltpu.VMEM((widths, count), jnp.float32),
            pltpu.VMEM((2 * widths * GROUP, count * GROUP), jnp.bfloat16),
            pltpu.VMEM((n * groups, count, GROUP, WIDE), jnp.bfloat16),
            pltpu.VMEM((n, groups, widths, GROUP, WIDE), jnp.float32),
            pltpu.VMEM((2, steps, widths, GROUP, WIDE), jnp.bfloat16),
            pltpu.VMEM((2, steps, 1, WIDE), jnp.float32),
            pltpu.VMEM((2, steps, widths, GROUP, WIDE), jnp.bfloat16),
            pltpu.VMEM((2, steps, 1, WIDE), jnp.float32),
            pltpu.VMEM((widths, 8, WIDE), jnp.float32),
            pltpu.VMEM((n * peers, 1, 128), jnp.float32),
            dma, dma((n * groups,)),
            dma((2, steps)), dma((2, steps)), dma((2, steps)), dma((2, steps)),
            dma((n * peers,)), dma((n * peers,)), regular, regular, regular, regular,
        ],
        compiler_params=pltpu.CompilerParams(
            collective_id=0, has_side_effects=True, vmem_limit_bytes=48 * 1024 * 1024
        ),
        name="reconstruct",
    )(coeffs, snapshots)
    return averages, norms[0, :widths]


def solution(mesh):
    in_specs = (P("snap", "param", None), P(None, "snap"))
    out_specs = (P(None, "param", "snap"), P())
    body = functools.partial(on_device, mesh.shape["snap"], mesh.shape["param"])
    return jax.shard_map(body, mesh=mesh, in_specs=in_specs, out_specs=out_specs, check_vma=False)
```

```python
import functools

import jax
import jax.numpy as jnp
from jax import lax
from jax.experimental import pallas as pl
from jax.experimental.pallas import tpu as pltpu
from jax.sharding import PartitionSpec as P

MESH = pl.DeviceIdType.MESH
GROUP = 16
WIDE = 128
LAG = 3
LATE = 5
HOLD_FIRST = 3
HOLD_FINAL = 5
HEAD = 6
POWER = 15
AHEAD = 2
TOP = 2.0**8.375


def encode(value):
    largest = jnp.max(jnp.max(jnp.abs(value), axis=0), axis=0, keepdims=True)
    largest = jnp.maximum(largest, 1e-30)
    x = value * (TOP / largest)[None]
    x2 = x * x
    x4 = x2 * x2
    x8 = x4 * x4
    return ((x8 * x4) * (x2 * x)).astype(jnp.bfloat16), largest * (1.0 / TOP)


def decode(code, scale):
    y = code.astype(jnp.float32)
    size = jnp.exp2(jnp.log2(jnp.maximum(jnp.abs(y), 1e-38)) * (1.0 / POWER)) * scale[None]
    return jnp.where(y > 0.0, size, jnp.where(y < 0.0, -size, 0.0))


def each(size, body):
    if size <= 8:
        for k in range(size):
            body(k)
    else:
        pl.loop(0, size)(body)


def shape_of(n, height, keep):
    cuts = keep // WIDE
    groups = height // GROUP * cuts
    lag = min(LAG, groups - 1)
    late = max(0, min(LATE, groups - lag, (n - 3) * (groups - lag)))
    return cuts, groups, (n - 1) * groups, lag, late


def kernel(
    n, peers, entries, coeffs, stored, averages, norms,
    weights, spread, tiles, part, out_code, out_scale, in_code, in_scale, squares, lines, result, both_sizes,
    coeff_sem, load_sem, write_sem, hand_sem, send_sem, send_scale_sem, recv_sem, line_send, line_recv,
    known, token_up, token_down, complete,
):
    z = lax.axis_index("snap")
    me = lax.axis_index("param")
    widths, count = coeffs.shape
    keep = stored.shape[2] // n
    cuts, groups, steps, lag, late = shape_of(n, stored.shape[1], keep)
    total = n * groups // cuts
    ring = load_sem.shape[0]
    low = z < n // 2
    first, final = z == 0, z == n - 1
    end = jnp.logical_or(first, final)
    middle = jnp.logical_not(end)
    hub = middle if n > 2 else end
    head = min(HEAD, total)

    def turned(d, s, last):
        return jnp.where(d == last, groups - 1 - s, s) if late > 0 else s

    def upwards(k):
        d = n - 1 - k // groups
        return d, turned(d, lax.rem(k, groups), n - 2)

    def downwards(k):
        d = k // groups
        return d, turned(d, lax.rem(k, groups), 1)

    def own(i):
        mixed = jnp.where(end, i, i // 2) if n % 2 == 0 else i
        rising = jnp.where(end, low, lax.rem(i, 2) == 0) if n % 2 == 0 else low
        du, tu = upwards(mixed * cuts)
        dd, td = downwards(mixed * cuts)
        return jnp.where(rising, du, dd), jnp.where(rising, tu, td)

    def load(i):
        d, t = own(i)
        return pltpu.make_async_copy(
            stored.at[:, pl.ds(pl.multiple_of(t // cuts * GROUP, GROUP), GROUP), pl.ds(pl.multiple_of(d * keep, keep), keep)],
            tiles.at[i],
            load_sem.at[lax.rem(i, ring)],
        )

    load(0).start()
    read = pltpu.make_async_copy(coeffs, weights, coeff_sem)
    read.start()
    barrier = pltpu.get_barrier_semaphore()

    @pl.when(z > 0)
    def _():
        pl.semaphore_signal(barrier, inc=1, device_id={"snap": z - 1}, device_id_type=MESH)

    @pl.when(z < n - 1)
    def _():
        pl.semaphore_signal(barrier, inc=1, device_id={"snap": z + 1}, device_id_type=MESH)

    def to_peers(semaphore):
        def body(k):
            @pl.when(k != me)
            def _():
                pl.semaphore_signal(semaphore, inc=1, device_id={"param": k}, device_id_type=MESH)

        each(peers, body)

    @pl.when(hub)
    def _():
        to_peers(barrier)

    tall, wide = spread.shape
    row = lax.broadcasted_iota(jnp.int32, (count, wide), 0)
    col = lax.broadcasted_iota(jnp.int32, (count, wide), 1)
    repeat = jnp.where(col // GROUP == row, 1.0, 0.0).astype(jnp.bfloat16)
    row = lax.broadcasted_iota(jnp.int32, (GROUP, wide), 0)
    col = lax.broadcasted_iota(jnp.int32, (GROUP, wide), 1)
    same = (row == col % GROUP)[None]
    read.wait()
    whole = weights[...]
    high = whole.astype(jnp.bfloat16)
    rest = (whole - high.astype(jnp.float32)).astype(jnp.bfloat16)
    both = jnp.concatenate([high, rest], axis=0)
    full = jnp.dot(both, repeat, preferred_element_type=jnp.float32)
    full = jnp.where(same, full[:, None, :], 0.0)
    spread[...] = full.reshape(tall, wide).astype(jnp.bfloat16)
    squares[...] = jnp.zeros_like(squares)

    def copies(way, k, peer):
        code = pltpu.make_async_remote_copy(
            src_ref=out_code.at[way, k], dst_ref=in_code.at[way, k],
            send_sem=send_sem.at[way], recv_sem=recv_sem.at[way, k],
            device_id={"snap": peer}, device_id_type=MESH,
        )
        scale = pltpu.make_async_remote_copy(
            src_ref=out_scale.at[way, k], dst_ref=in_scale.at[way, k],
            send_sem=send_scale_sem.at[way], recv_sem=recv_sem.at[way, k],
            device_id={"snap": peer}, device_id_type=MESH,
        )
        return scale, code

    def launch(way, k, peer):
        for copy in copies(way, k, peer):
            copy.start()

    def pack(way, k, value):
        code, scale = encode(value)
        out_code[way, k] = code
        out_scale[way, k] = scale

    def send(way, k, peer, value):
        pack(way, k, value)
        launch(way, k, peer)

    def arrived(way, k):
        pltpu.make_async_copy(both_sizes, both_sizes, recv_sem.at[way, k]).wait()
        return decode(in_code[way, k], in_scale[way, k])

    def count_squares(value):
        squares[...] += jnp.sum((value * value).reshape(widths, GROUP // 8, 8, WIDE), axis=1)

    half = widths * GROUP

    def multiply(i):
        d, t = own(i)
        load(i).wait()

        @pl.when(i + AHEAD < total)
        def _():
            load(i + AHEAD).start()

        both_parts = jnp.dot(
            spread[...], tiles[i].reshape(count * GROUP, keep), preferred_element_type=jnp.float32
        )
        value = (both_parts[:half] + both_parts[half:]).reshape(widths, GROUP, keep)
        pieces = [value[:, :, c * WIDE:(c + 1) * WIDE] for c in range(cuts)]
        for c, piece in enumerate(pieces):
            part[d, t // cuts * cuts + c] = piece
        return d, t, pieces

    for i in range(1, min(AHEAD, total)):
        load(i).start()

    ends_way = jnp.where(first, 0, 1)
    ends_peer = jnp.where(first, 1, n - 2)
    if late > 0:
        held = steps - jnp.where(first, HOLD_FIRST, HOLD_FINAL)
    else:
        held = steps

    @pl.when(end)
    def _():
        @pl.loop(0, total)
        def _(i):
            d, t, pieces = multiply(i)

            @pl.when(i == 0)
            def _():
                pl.semaphore_wait(barrier, 1 if n > 2 else peers)

            @pl.when(d != z)
            def _():
                back = lax.rem(t, cuts) > 0
                for c, piece in enumerate(pieces):
                    k = i * cuts + jnp.where(back, cuts - 1 - c, c)
                    pack(ends_way, k, piece)

                    @pl.when(k < held)
                    def _():
                        launch(ends_way, k, ends_peer)

        if n == 2:
            to_peers(known)
            pl.semaphore_wait(known, peers - 1)

    def write(t):
        rows = pl.ds(pl.multiple_of(t // cuts * GROUP, GROUP), GROUP)
        columns = pl.ds(pl.multiple_of(lax.rem(t, cuts) * WIDE, WIDE), WIDE)
        return pltpu.make_async_copy(part.at[z, t], averages.at[:, rows, columns], write_sem)

    def settle(t, value):
        part[z, t] = value
        write(t).start()

    def both_ways(t, value, second, counted):
        @pl.when(second)
        def _():
            settle(t, value)

            @pl.when(counted)
            def _():
                count_squares(value)

        @pl.when(jnp.logical_not(second))
        def _():
            part[z, t] = value

    def pass_on(j):
        up = j - lag * (z - 1)
        down = j - lag * (n - 2 - z)

        @pl.when(jnp.logical_and(up >= 0, up < (n - z) * groups))
        def _():
            d, t = upwards(up)
            value = part[d, t] + arrived(0, up)

            @pl.when(d == z)
            def _():
                s = turned(z, t, 1)
                second = z * groups + s + lag * (n - 2 - z) < j
                both_ways(t, value, second, jnp.logical_or(z != 1, t < groups - late))

            extra = jnp.logical_and(z == n - 2, up < groups + late) if late > 0 else False

            @pl.when(jnp.logical_or(d != z, extra))
            def _():
                send(0, up, z + 1, value)

        @pl.when(jnp.logical_and(down >= 0, down < (z + 1) * groups))
        def _():
            d, t = downwards(down)
            value = part[d, t] + arrived(1, down)

            @pl.when(d == z)
            def _():
                s = turned(z, t, n - 2)
                second = (n - 1 - z) * groups + s + lag * (z - 1) <= j
                both_ways(t, value, second, jnp.logical_or(z != n - 2, t < groups - late))

            extra = jnp.logical_and(z == 1, down < groups + late) if late > 0 else False

            @pl.when(jnp.logical_or(d != z, extra))
            def _():
                send(1, down, z - 1, value)

    @pl.when(middle)
    def _():
        pl.loop(0, head)(lambda i: multiply(i) and None)
        pl.semaphore_wait(barrier, 2 + peers - 1)
        to_peers(known)

        @pl.loop(0, steps - late)
        def _(j):
            pass_on(j)

            @pl.when(j + head < total)
            def _():
                multiply(j + head)

            @pl.when(j == 2)
            def _():
                pl.semaphore_wait(known, peers - 1)

                @pl.when(z > 1)
                def _():
                    pl.semaphore_signal(token_down, inc=1, device_id={"snap": z - 1}, device_id_type=MESH)

                @pl.when(z < n - 2)
                def _():
                    pl.semaphore_signal(token_up, inc=1, device_id={"snap": z + 1}, device_id_type=MESH)

            @pl.when(j == 4)
            def _():
                @pl.when(z > 1)
                def _():
                    pl.semaphore_wait(token_up, 1)

                @pl.when(z < n - 2)
                def _():
                    pl.semaphore_wait(token_down, 1)

                @pl.when(z == 1)
                def _():
                    pl.semaphore_signal(complete, inc=1, device_id={"snap": z - 1}, device_id_type=MESH)

                @pl.when(z == n - 2)
                def _():
                    pl.semaphore_signal(complete, inc=1, device_id={"snap": z + 1}, device_id_type=MESH)

    @pl.when(end)
    def _():
        @pl.loop(0, groups + late)
        def _(k):
            t = jnp.where(k < groups, k, 2 * groups - 1 - k)
            d = jnp.where(k < groups, z, ends_peer)
            value = part[d, t] + arrived(1 - ends_way, k)
            count_squares(value)

            @pl.when(k < groups)
            def _():
                settle(t, value)

        if n > 2:
            pl.semaphore_wait(complete, 1)

    sums = jnp.sum(jnp.sum(squares[...], axis=1), axis=1, keepdims=True)
    lanes = norms.shape[1]
    row = lax.broadcasted_iota(jnp.int32, (widths, lanes), 0)
    col = lax.broadcasted_iota(jnp.int32, (widths, lanes), 1)
    line = jnp.sum(jnp.where(row == col, sums, 0.0), axis=0, keepdims=True)

    mine = z * peers + me
    lines[mine] = line

    for p in range(n):
        def body(k, p=p):
            @pl.when(jnp.logical_or(p != z, k != me))
            def _():
                pltpu.make_async_remote_copy(
                    src_ref=lines.at[mine], dst_ref=lines.at[mine], send_sem=line_send, recv_sem=line_recv,
                    device_id={"snap": p, "param": k}, device_id_type=MESH,
                ).start()

        each(peers, body)

    if late > 0:
        @pl.when(end)
        def _():
            pl.loop(held, steps)(lambda k: launch(ends_way, k, ends_peer))

        @pl.when(middle)
        def _():
            pl.loop(steps - late, steps - 1)(pass_on)

    def sent(way, amount):
        if amount > 0:
            some = pl.ds(0, amount)
            pltpu.make_async_copy(out_code.at[way, some], out_code.at[way, some], send_sem.at[way]).wait()
            pltpu.make_async_copy(out_scale.at[way, some], out_scale.at[way, some], send_scale_sem.at[way]).wait()

    def all_sent(layers):
        for layer in layers:
            @pl.when(z == layer)
            def _(layer=layer):
                sent(0, (n - 1 - layer) * groups + (late if layer == n - 2 else 0))
                sent(1, layer * groups + (late if layer == 1 else 0))

    all_sent(range(1, n - 1))
    rest_of = lines.at[pl.ds(0, n * peers - 1)]
    pltpu.make_async_copy(rest_of, rest_of, line_send).wait()
    pltpu.make_async_copy(rest_of, rest_of, line_recv).wait()
    result[...] = jnp.sqrt(jnp.sum(lines[...], axis=0) / jnp.float32(entries))
    hand = pltpu.make_async_copy(result, norms, hand_sem)
    hand.start()

    if late > 0:
        @pl.when(middle)
        def _():
            pass_on(steps - 1)

    all_sent((0, n - 1))
    pltpu.make_async_copy(averages, averages, write_sem).wait()
    hand.wait()


def on_device(n, peers, snapshots, coeffs):
    count, height, cols = snapshots.shape
    widths = coeffs.shape[0]
    keep = cols // n
    cuts, groups, steps, lag, late = shape_of(n, height, keep)
    total = n * groups // cuts
    entries = height * cols * peers
    dma = pltpu.SemaphoreType.DMA
    regular = pltpu.SemaphoreType.REGULAR
    averages, norms = pl.pallas_call(
        functools.partial(kernel, n, peers, entries),
        out_shape=(
            jax.ShapeDtypeStruct((widths, height, keep), jnp.float32),
            jax.ShapeDtypeStruct((1, 128), jnp.float32),
        ),
        in_specs=[pl.BlockSpec(memory_space=pl.ANY), pl.BlockSpec(memory_space=pl.ANY)],
        out_specs=(pl.BlockSpec(memory_space=pl.ANY), pl.BlockSpec(memory_space=pl.ANY)),
        scratch_shapes=[
            pltpu.VMEM((widths, count), jnp.float32),
            pltpu.VMEM((2 * widths * GROUP, count * GROUP), jnp.bfloat16),
            pltpu.VMEM((total, count, GROUP, keep), jnp.bfloat16),
            pltpu.VMEM((n, groups, widths, GROUP, WIDE), jnp.float32),
            pltpu.VMEM((2, steps, widths, GROUP, WIDE), jnp.bfloat16),
            pltpu.VMEM((2, steps, 1, WIDE), jnp.float32),
            pltpu.VMEM((2, steps, widths, GROUP, WIDE), jnp.bfloat16),
            pltpu.VMEM((2, steps, 1, WIDE), jnp.float32),
            pltpu.VMEM((widths, 8, WIDE), jnp.float32),
            pltpu.VMEM((n * peers, 1, 128), jnp.float32),
            pltpu.VMEM((1, 128), jnp.float32),
            pltpu.VMEM((widths * GROUP // 2 + 1, 1, WIDE), jnp.float32),
            dma, dma((AHEAD + 1,)), dma, dma, dma((2,)), dma((2,)), dma((2, steps)), dma, dma,
            regular, regular, regular, regular,
        ],
        compiler_params=pltpu.CompilerParams(
            collective_id=0, has_side_effects=True, vmem_limit_bytes=48 * 1024 * 1024
        ),
        name="reconstruct",
    )(coeffs, snapshots)
    return averages, norms[0, :widths]


def solution(mesh):
    in_specs = (P("snap", "param", None), P(None, "snap"))
    out_specs = (P(None, "param", "snap"), P())
    body = functools.partial(on_device, mesh.shape["snap"], mesh.shape["param"])
    return jax.shard_map(body, mesh=mesh, in_specs=in_specs, out_specs=out_specs, check_vma=False)
```

```python
import functools

import jax
import jax.numpy as jnp
from jax import lax
from jax.experimental import pallas as pl
from jax.experimental.pallas import tpu as pltpu
from jax.sharding import PartitionSpec as P

MESH = pl.DeviceIdType.MESH
GROUP = 16
WIDE = 128
LAG_UP = 3
LAG_DOWN = 4
LATE = 5
HOLD_FIRST = 3
HOLD_FINAL = 4
KEEP_FIRST = 3
KEEP_FINAL = 4
HEAD = 6
POWER = 15
AHEAD = 2
SPLIT = 1
TOP = 2.0**8.375


def encode(value):
    largest = jnp.max(jnp.max(jnp.abs(value), axis=0), axis=0, keepdims=True)
    largest = jnp.maximum(largest, 1e-30)
    x = value * (TOP / largest)[None]
    x2 = x * x
    x4 = x2 * x2
    x8 = x4 * x4
    return ((x8 * x4) * (x2 * x)).astype(jnp.bfloat16), largest * (1.0 / TOP)


def decode(code, scale):
    y = code.astype(jnp.float32)
    size = jnp.exp2(jnp.log2(jnp.maximum(jnp.abs(y), 1e-38)) * (1.0 / POWER)) * scale[None]
    return jnp.where(y > 0.0, size, jnp.where(y < 0.0, -size, 0.0))


def each(size, body):
    if size <= 8:
        for k in range(size):
            body(k)
    else:
        pl.loop(0, size)(body)


def shape_of(n, height, keep):
    cuts = keep // WIDE
    groups = height // GROUP * cuts
    lags = min(LAG_UP, groups - 1), min(LAG_DOWN, groups - 1)
    late = min(LATE, groups - 1) if n > 3 else 0
    return cuts, groups, (n - 1) * groups, lags, late


def kernel(
    n, peers, entries, coeffs, stored, averages, norms,
    weights, spread, tiles, part, out_code, out_scale, in_code, in_scale, squares, lines, result, both_sizes,
    coeff_sem, load_sem, write_sem, hand_sem, send_sem, send_scale_sem, recv_sem, line_send, line_recv,
    known, token_up, token_down, complete,
):
    z = lax.axis_index("snap")
    me = lax.axis_index("param")
    widths, count = coeffs.shape
    keep = stored.shape[2] // n
    cuts, groups, steps, (lag_up, lag_down), late = shape_of(n, stored.shape[1], keep)
    total = n * groups // cuts
    ring = load_sem.shape[0]
    low = z < n // 2
    first, final = z == 0, z == n - 1
    end = jnp.logical_or(first, final)
    middle = jnp.logical_not(end)
    hub = middle if n > 2 else end
    head = min(HEAD, total)
    more = max(1, 2 // cuts)

    def turned(d, s, last):
        return jnp.where(d == last, groups - 1 - s, s) if late > 0 else s

    def upwards(k):
        d = n - 1 - k // groups
        return d, turned(d, lax.rem(k, groups), n - 2)

    def downwards(k):
        d = k // groups
        return d, turned(d, lax.rem(k, groups), 1)

    def own(i):
        mixed = jnp.where(end, i, i // 2) if n % 2 == 0 else i
        rising = jnp.where(end, low, lax.rem(i, 2) == 0) if n % 2 == 0 else low
        du, tu = upwards(mixed * cuts)
        dd, td = downwards(mixed * cuts)
        return jnp.where(rising, du, dd), jnp.where(rising, tu, td)

    def load(i):
        d, t = own(i)
        return pltpu.make_async_copy(
            stored.at[:, pl.ds(pl.multiple_of(t // cuts * GROUP, GROUP), GROUP), pl.ds(pl.multiple_of(d * keep, keep), keep)],
            tiles.at[i],
            load_sem.at[lax.rem(i, ring)],
        )

    read = pltpu.make_async_copy(coeffs, weights, coeff_sem)
    read.start()
    load(0).start()
    barrier = pltpu.get_barrier_semaphore()

    @pl.when(z > 0)
    def _():
        pl.semaphore_signal(barrier, inc=1, device_id={"snap": z - 1}, device_id_type=MESH)

    @pl.when(z < n - 1)
    def _():
        pl.semaphore_signal(barrier, inc=1, device_id={"snap": z + 1}, device_id_type=MESH)

    def to_peers(semaphore):
        def body(k):
            @pl.when(k != me)
            def _():
                pl.semaphore_signal(semaphore, inc=1, device_id={"param": k}, device_id_type=MESH)

        each(peers, body)

    @pl.when(hub)
    def _():
        to_peers(barrier)

    tall, wide = spread.shape
    row = lax.broadcasted_iota(jnp.int32, (count, wide), 0)
    col = lax.broadcasted_iota(jnp.int32, (count, wide), 1)
    repeat = jnp.where(col // GROUP == row, 1.0, 0.0).astype(jnp.bfloat16)
    row = lax.broadcasted_iota(jnp.int32, (GROUP, wide), 0)
    col = lax.broadcasted_iota(jnp.int32, (GROUP, wide), 1)
    same = (row == col % GROUP)[None]
    read.wait()
    whole = weights[...]
    high = whole.astype(jnp.bfloat16)
    rest = (whole - high.astype(jnp.float32)).astype(jnp.bfloat16)
    both = jnp.concatenate([high, rest], axis=0)
    full = jnp.dot(both, repeat, preferred_element_type=jnp.float32)
    full = jnp.where(same, full[:, None, :], 0.0)
    spread[...] = full.reshape(tall, wide).astype(jnp.bfloat16)
    squares[...] = jnp.zeros_like(squares)

    def copies(way, k, peer):
        code = pltpu.make_async_remote_copy(
            src_ref=out_code.at[way, k], dst_ref=in_code.at[way, k],
            send_sem=send_sem.at[way], recv_sem=recv_sem.at[way, k],
            device_id={"snap": peer}, device_id_type=MESH,
        )
        scale = pltpu.make_async_remote_copy(
            src_ref=out_scale.at[way, k], dst_ref=in_scale.at[way, k],
            send_sem=send_scale_sem.at[way], recv_sem=recv_sem.at[way, k],
            device_id={"snap": peer}, device_id_type=MESH,
        )
        return scale, code

    def launch(way, k, peer):
        for copy in copies(way, k, peer):
            copy.start()

    def pack(way, k, value):
        code, scale = encode(value)
        out_code[way, k] = code
        out_scale[way, k] = scale

    def send(way, k, peer, value):
        pack(way, k, value)
        launch(way, k, peer)

    def arrived(way, k):
        pltpu.make_async_copy(both_sizes, both_sizes, recv_sem.at[way, k]).wait()
        return decode(in_code[way, k], in_scale[way, k])

    def count_squares(value):
        squares[...] += jnp.sum((value * value).reshape(widths, GROUP // 8, 8, WIDE), axis=1)

    half = widths * GROUP

    def multiply(i):
        d, t = own(i)
        load(i).wait()

        @pl.when(i + AHEAD < total)
        def _():
            load(i + AHEAD).start()

        both_parts = jnp.dot(
            spread[...], tiles[i].reshape(count * GROUP, keep), preferred_element_type=jnp.float32
        )
        value = (both_parts[:half] + both_parts[half:]).reshape(widths, GROUP, keep)
        pieces = [value[:, :, c * WIDE:(c + 1) * WIDE] for c in range(cuts)]
        for c, piece in enumerate(pieces):
            part[d, t // cuts * cuts + c] = piece
        return d, t, pieces

    for i in range(1, min(AHEAD, total)):
        load(i).start()

    ends_way = jnp.where(first, 0, 1)
    ends_peer = jnp.where(first, 1, n - 2)
    if late > 0:
        held = steps - jnp.where(first, HOLD_FIRST, HOLD_FINAL)
        kept = steps - jnp.where(first, KEEP_FIRST, KEEP_FINAL)
    else:
        held = steps

    @pl.when(end)
    def _():
        @pl.loop(0, total)
        def _(i):
            d, t, pieces = multiply(i)

            @pl.when(i == 0)
            def _():
                pl.semaphore_wait(barrier, 1 if n > 2 else peers)

            @pl.when(d != z)
            def _():
                back = lax.rem(t, cuts) > 0
                for c in range(cuts):
                    k = i * cuts + c
                    pack(ends_way, k, jnp.where(back, pieces[cuts - 1 - c], pieces[c]))

                    @pl.when(k < held)
                    def _():
                        launch(ends_way, k, ends_peer)

        if n == 2:
            to_peers(known)
            pl.semaphore_wait(known, peers - 1)

    def write(t):
        rows = pl.ds(pl.multiple_of(t // cuts * GROUP, GROUP), GROUP)
        columns = pl.ds(pl.multiple_of(lax.rem(t, cuts) * WIDE, WIDE), WIDE)
        return pltpu.make_async_copy(part.at[z, t], averages.at[:, rows, columns], write_sem)

    def settle(t, value):
        part[z, t] = value
        write(t).start()

    def both_ways(t, value, second, counted):
        @pl.when(second)
        def _():
            settle(t, value)

            @pl.when(counted)
            def _():
                count_squares(value)

        @pl.when(jnp.logical_not(second))
        def _():
            part[z, t] = value

    up_delay = lag_up * (z - 1)
    down_delay = lag_down * (n - 2 - z)

    def pass_up(up):
        @pl.when(jnp.logical_and(up >= 0, up < (n - z) * groups))
        def _():
            d, t = upwards(up)
            value = part[d, t] + arrived(0, up)

            @pl.when(d == z)
            def _():
                s = turned(z, t, 1)
                second = z * groups + s + down_delay < up + up_delay
                both_ways(t, value, second, jnp.logical_or(z != 1, t < groups - late))

            extra = jnp.logical_and(z == n - 2, up < groups + late) if late > 0 else False

            @pl.when(jnp.logical_or(d != z, extra))
            def _():
                send(0, up, z + 1, value)

    def pass_down(down):
        @pl.when(jnp.logical_and(down >= 0, down < (z + 1) * groups))
        def _():
            d, t = downwards(down)
            value = part[d, t] + arrived(1, down)

            @pl.when(d == z)
            def _():
                s = turned(z, t, n - 2)
                second = (n - 1 - z) * groups + s + up_delay <= down + down_delay
                both_ways(t, value, second, jnp.logical_or(z != n - 2, t < groups - late))

            extra = jnp.logical_and(z == 1, down < groups + late) if late > 0 else False

            @pl.when(jnp.logical_or(d != z, extra))
            def _():
                send(1, down, z - 1, value)

    def pass_on(j):
        pass_up(j - up_delay)
        pass_down(j - down_delay)

    @pl.when(middle)
    def _():
        pl.loop(0, head)(lambda i: multiply(i) and None)
        pl.semaphore_wait(barrier, 2 + peers - 1)
        to_peers(known)

        @pl.loop(0, steps - late)
        def _(j):
            pass_on(j)

            for m in range(more):
                @pl.when(more * j + m + head < total)
                def _(m=m):
                    multiply(more * j + m + head)

            @pl.when(j == 2)
            def _():
                pl.semaphore_wait(known, peers - 1)

                @pl.when(z > 1)
                def _():
                    pl.semaphore_signal(token_down, inc=1, device_id={"snap": z - 1}, device_id_type=MESH)

                @pl.when(z < n - 2)
                def _():
                    pl.semaphore_signal(token_up, inc=1, device_id={"snap": z + 1}, device_id_type=MESH)

            @pl.when(j == 4)
            def _():
                @pl.when(z > 1)
                def _():
                    pl.semaphore_wait(token_up, 1)

                @pl.when(z < n - 2)
                def _():
                    pl.semaphore_wait(token_down, 1)

                @pl.when(z == 1)
                def _():
                    pl.semaphore_signal(complete, inc=1, device_id={"snap": z - 1}, device_id_type=MESH)

                @pl.when(z == n - 2)
                def _():
                    pl.semaphore_signal(complete, inc=1, device_id={"snap": z + 1}, device_id_type=MESH)

    if late > 0:
        @pl.when(z == 1)
        def _():
            pl.loop(steps - late - down_delay, 2 * groups)(pass_down)

        @pl.when(z == n - 2)
        def _():
            pl.loop(steps - late - up_delay, 2 * groups)(pass_up)

    @pl.when(end)
    def _():
        @pl.loop(0, groups + late)
        def _(k):
            if late > 0:
                early = k - (groups + late) + (kept - held)

                @pl.when(early >= 0)
                def _():
                    launch(ends_way, held + early, ends_peer)

            t = jnp.where(k < groups, k, 2 * groups - 1 - k)
            d = jnp.where(k < groups, z, ends_peer)
            value = part[d, t] + arrived(1 - ends_way, k)
            count_squares(value)

            @pl.when(k < groups)
            def _():
                settle(t, value)

        if n > 2:
            pl.semaphore_wait(complete, 1)

    sums = jnp.sum(jnp.sum(squares[...], axis=1), axis=1, keepdims=True)
    lanes = norms.shape[1]
    row = lax.broadcasted_iota(jnp.int32, (widths, lanes), 0)
    col = lax.broadcasted_iota(jnp.int32, (widths, lanes), 1)
    line = jnp.sum(jnp.where(row == col, sums, 0.0), axis=0, keepdims=True)

    mine = z * peers + me
    lines[mine] = line

    for p in range(n):
        def body(k, p=p):
            @pl.when(jnp.logical_or(p != z, k != me))
            def _():
                pltpu.make_async_remote_copy(
                    src_ref=lines.at[mine], dst_ref=lines.at[mine], send_sem=line_send, recv_sem=line_recv,
                    device_id={"snap": p, "param": k}, device_id_type=MESH,
                ).start()

        each(peers, body)

    if late > 0:
        @pl.when(end)
        def _():
            pl.loop(kept, steps)(lambda k: launch(ends_way, k, ends_peer))

        @pl.when(z == 1)
        def _():
            pl.loop(steps - late, steps - 1)(pass_up)

        @pl.when(z == n - 2)
        def _():
            pl.loop(steps - late, steps - 1)(pass_down)

    def sent(way, amount):
        if amount > 0:
            some = pl.ds(0, amount)
            pltpu.make_async_copy(out_code.at[way, some], out_code.at[way, some], send_sem.at[way]).wait()
            pltpu.make_async_copy(out_scale.at[way, some], out_scale.at[way, some], send_scale_sem.at[way]).wait()

    def all_sent(layers):
        for layer in layers:
            @pl.when(z == layer)
            def _(layer=layer):
                sent(0, (n - 1 - layer) * groups + (late if layer == n - 2 else 0))
                sent(1, layer * groups + (late if layer == 1 else 0))

    all_sent(range(1, n - 1))
    rest_of = lines.at[pl.ds(0, n * peers - 1)]
    pltpu.make_async_copy(rest_of, rest_of, line_send).wait()
    pltpu.make_async_copy(rest_of, rest_of, line_recv).wait()
    result[...] = jnp.sqrt(jnp.sum(lines[...], axis=0) / jnp.float32(entries))
    hand = pltpu.make_async_copy(result, norms, hand_sem)
    hand.start()

    if late > 0:
        @pl.when(z == 1)
        def _():
            pass_up(steps - 1)

        @pl.when(z == n - 2)
        def _():
            pass_down(steps - 1)

    all_sent((0, n - 1))
    pltpu.make_async_copy(averages, averages, write_sem).wait()
    hand.wait()


def hand_out(averages, norms, widths):
    def body(averages, norms, averages_out, norms_out, line, row, sems):
        parts = SPLIT
        size = averages.shape[0] // parts


        for k in range(parts):
            some = pl.ds(k * size, size)
            pltpu.make_async_copy(averages.at[some], averages_out.at[some], sems.at[k]).start()

        row[...] = norms[0, :widths]
        write = pltpu.make_async_copy(row, norms_out, sems.at[parts])
        write.start()
        for k in range(parts):
            some = pl.ds(k * size, size)
            pltpu.make_async_copy(averages.at[some], averages_out.at[some], sems.at[k]).wait()
        write.wait()

    anywhere = pl.BlockSpec(memory_space=pl.ANY)
    return pl.pallas_call(
        body,
        out_shape=(
            jax.ShapeDtypeStruct(averages.shape, jnp.float32),
            jax.ShapeDtypeStruct((widths,), jnp.float32),
        ),
        in_specs=[pl.BlockSpec(memory_space=pltpu.VMEM)] * 2,
        out_specs=(anywhere, anywhere),
        scratch_shapes=[pltpu.VMEM((1, 128), jnp.float32), pltpu.VMEM((widths,), jnp.float32), pltpu.SemaphoreType.DMA((SPLIT + 1,))],
        name="hand_out",
    )(pltpu.with_memory_space_constraint(averages, pltpu.VMEM), pltpu.with_memory_space_constraint(norms, pltpu.VMEM))


def on_device(n, peers, snapshots, coeffs):
    count, height, cols = snapshots.shape
    widths = coeffs.shape[0]
    keep = cols // n
    cuts, groups, steps, lags, late = shape_of(n, height, keep)
    total = n * groups // cuts
    entries = height * cols * peers
    dma = pltpu.SemaphoreType.DMA
    regular = pltpu.SemaphoreType.REGULAR
    averages, norms = pl.pallas_call(
        functools.partial(kernel, n, peers, entries),
        out_shape=(
            jax.ShapeDtypeStruct((widths, height, keep), jnp.float32),
            jax.ShapeDtypeStruct((1, 128), jnp.float32),
        ),
        in_specs=[pl.BlockSpec(memory_space=pl.ANY), pl.BlockSpec(memory_space=pl.ANY)],
        out_specs=(pl.BlockSpec(memory_space=pl.ANY), pl.BlockSpec(memory_space=pl.ANY)),
        scratch_shapes=[
            pltpu.VMEM((widths, count), jnp.float32),
            pltpu.VMEM((2 * widths * GROUP, count * GROUP), jnp.bfloat16),
            pltpu.VMEM((total, count, GROUP, keep), jnp.bfloat16),
            pltpu.VMEM((n, groups, widths, GROUP, WIDE), jnp.float32),
            pltpu.VMEM((2, steps, widths, GROUP, WIDE), jnp.bfloat16),
            pltpu.VMEM((2, steps, 1, WIDE), jnp.float32),
            pltpu.VMEM((2, steps, widths, GROUP, WIDE), jnp.bfloat16),
            pltpu.VMEM((2, steps, 1, WIDE), jnp.float32),
            pltpu.VMEM((widths, 8, WIDE), jnp.float32),
            pltpu.VMEM((n * peers, 1, 128), jnp.float32),
            pltpu.VMEM((1, 128), jnp.float32),
            pltpu.VMEM((widths * GROUP // 2 + 1, 1, WIDE), jnp.float32),
            dma, dma((AHEAD + 1,)), dma, dma, dma((2,)), dma((2,)), dma((2, steps)), dma, dma,
            regular, regular, regular, regular,
        ],
        compiler_params=pltpu.CompilerParams(
            collective_id=0, has_side_effects=True, vmem_limit_bytes=48 * 1024 * 1024
        ),
        name="reconstruct",
    )(pltpu.with_memory_space_constraint(coeffs, pltpu.HBM), snapshots)
    return hand_out(averages, norms, widths)


def solution(mesh):
    in_specs = (P("snap", "param", None), P(None, "snap"))
    out_specs = (P(None, "param", "snap"), P())
    body = functools.partial(on_device, mesh.shape["snap"], mesh.shape["param"])
    return jax.shard_map(body, mesh=mesh, in_specs=in_specs, out_specs=out_specs, check_vma=False)
```

```python
import functools
import math

import jax
import jax.numpy as jnp
from jax import lax
from jax.experimental import pallas as pl
from jax.experimental.pallas import tpu as pltpu
from jax.sharding import PartitionSpec as P

MESH = pl.DeviceIdType.MESH
GROUP = 8
LAG_UP = 2
LAG_DOWN = 3
LATE = 6
HOLD_FIRST = 3
HOLD_FINAL = 4
KEEP_FIRST = 3
KEEP_FINAL = 4
HEAD = 10
POWER = 15
AHEAD = 3
SPLIT = 1
SPLIT_FIRST = 1
TOP = 2.0**8.375
LANES = 128


def encode(value):
    lanes = [value[:, c:c + LANES] for c in range(0, value.shape[1], LANES)]
    largest = functools.reduce(jnp.maximum, [jnp.abs(lane) for lane in lanes])
    largest = jnp.maximum(jnp.max(largest, axis=0, keepdims=True), 1e-30)
    x = value * jnp.concatenate([TOP / largest] * len(lanes), axis=1)
    x2 = x * x
    x4 = x2 * x2
    x8 = x4 * x4
    return ((x8 * x4) * (x2 * x)).astype(jnp.bfloat16), largest * (1.0 / TOP)


def decode(code, scale):
    y = code.astype(jnp.float32)
    scale = jnp.concatenate([scale] * (code.shape[1] // LANES), axis=1)
    size = jnp.exp2(jnp.log2(jnp.maximum(jnp.abs(y), 1e-38)) * (1.0 / POWER)) * scale
    return jnp.where(y > 0.0, size, jnp.where(y < 0.0, -size, 0.0))


def each(size, body):
    if size <= 8:
        for k in range(size):
            body(k)
    else:
        pl.loop(0, size)(body)


def shape_of(n, height):
    groups = height // GROUP
    lags = min(LAG_UP, groups - 1), min(LAG_DOWN, groups - 1)
    late = min(LATE, groups - 1) if n > 3 else 0
    return groups, (n - 1) * groups, lags, late


def kernel(
    n, peers, entries, coeffs, stored, averages, norms,
    weights, spread, tiles, part, out_code, out_scale, in_code, in_scale, squares, lines, result, both_sizes,
    coeff_sem, load_sem, write_sem, hand_sem, send_sem, send_scale_sem, recv_sem, line_send, line_recv,
    known, token_up, token_down, complete,
):
    z = lax.axis_index("snap")
    me = lax.axis_index("param")
    widths, count = coeffs.shape
    keep = stored.shape[2] // n
    groups, steps, (lag_up, lag_down), late = shape_of(n, stored.shape[1])
    total = n * groups
    ring = load_sem.shape[0]
    low = z < n // 2
    first, final = z == 0, z == n - 1
    end = jnp.logical_or(first, final)
    middle = jnp.logical_not(end)
    hub = middle if n > 2 else end
    head = min(HEAD, total)
    more = 2

    def turned(d, s, last):
        return jnp.where(d == last, groups - 1 - s, s) if late > 0 else s

    def upwards(k):
        d = n - 1 - k // groups
        return d, turned(d, lax.rem(k, groups), n - 2)

    def downwards(k):
        d = k // groups
        return d, turned(d, lax.rem(k, groups), 1)

    def own(i):
        mixed = jnp.where(end, i, i // 2) if n % 2 == 0 else i
        rising = jnp.where(end, low, lax.rem(i, 2) == 0) if n % 2 == 0 else low
        du, tu = upwards(mixed)
        dd, td = downwards(mixed)
        return jnp.where(rising, du, dd), jnp.where(rising, tu, td)

    def load(i, begin=0, amount=count):
        d, t = own(i)
        some = pl.ds(begin, amount)
        return pltpu.make_async_copy(
            stored.at[some, pl.ds(pl.multiple_of(t * GROUP, GROUP), GROUP), pl.ds(pl.multiple_of(d * keep, keep), keep)],
            tiles.at[i, some],
            load_sem.at[lax.rem(i, ring)],
        )

    read = pltpu.make_async_copy(coeffs, weights, coeff_sem)
    read.start()
    split = math.gcd(SPLIT_FIRST, count)
    for c in range(split):
        load(0, c * (count // split), count // split).start()
    barrier = pltpu.get_barrier_semaphore()

    @pl.when(z > 0)
    def _():
        pl.semaphore_signal(barrier, inc=1, device_id={"snap": z - 1}, device_id_type=MESH)

    @pl.when(z < n - 1)
    def _():
        pl.semaphore_signal(barrier, inc=1, device_id={"snap": z + 1}, device_id_type=MESH)

    def to_peers(semaphore):
        def body(k):
            @pl.when(k != me)
            def _():
                pl.semaphore_signal(semaphore, inc=1, device_id={"param": k}, device_id_type=MESH)

        each(peers, body)

    @pl.when(hub)
    def _():
        to_peers(barrier)

    tall, wide = spread.shape
    row = lax.broadcasted_iota(jnp.int32, (count, wide), 0)
    col = lax.broadcasted_iota(jnp.int32, (count, wide), 1)
    repeat = jnp.where(col // GROUP == row, 1.0, 0.0).astype(jnp.bfloat16)
    row = lax.broadcasted_iota(jnp.int32, (GROUP, wide), 0)
    col = lax.broadcasted_iota(jnp.int32, (GROUP, wide), 1)
    same = (row == col % GROUP)[None]
    read.wait()
    whole = weights[...]
    high = whole.astype(jnp.bfloat16)
    rest = (whole - high.astype(jnp.float32)).astype(jnp.bfloat16)
    both = jnp.concatenate([high, rest], axis=0)
    full = jnp.dot(both, repeat, preferred_element_type=jnp.float32)
    full = jnp.where(same, full[:, None, :], 0.0)
    spread[...] = full.reshape(tall, wide).astype(jnp.bfloat16)
    squares[...] = jnp.zeros_like(squares)

    def place(layer, way, k):
        return jnp.where(jnp.where(layer < n // 2, 0, 1) == way, k, steps + k)

    def copies(way, k, peer):
        code = pltpu.make_async_remote_copy(
            src_ref=out_code.at[way, k], dst_ref=in_code.at[way, k],
            send_sem=send_sem.at[way], recv_sem=recv_sem.at[place(peer, way, k)],
            device_id={"snap": peer}, device_id_type=MESH,
        )
        scale = pltpu.make_async_remote_copy(
            src_ref=out_scale.at[way, k], dst_ref=in_scale.at[way, k],
            send_sem=send_scale_sem.at[way], recv_sem=recv_sem.at[place(peer, way, k)],
            device_id={"snap": peer}, device_id_type=MESH,
        )
        return scale, code

    def launch(way, k, peer):
        for copy in copies(way, k, peer):
            copy.start()

    def pack(way, k, value):
        code, scale = encode(value.reshape(widths * GROUP, keep))
        out_code[way, k] = code
        out_scale[way, k] = scale

    def send(way, k, peer, value):
        pack(way, k, value)
        launch(way, k, peer)

    def arrived(way, k):
        pltpu.make_async_copy(both_sizes, both_sizes, recv_sem.at[place(z, way, k)]).wait()
        return decode(in_code[way, k], in_scale[way, k]).reshape(widths, GROUP, keep)

    def count_squares(value):
        square = value * value
        squares[...] += sum(square[:, :, c:c + LANES] for c in range(0, keep, LANES))

    half = widths * GROUP

    def multiply(i):
        d, t = own(i)
        load(i).wait()

        @pl.when(i + AHEAD < total)
        def _():
            load(i + AHEAD).start()

        both_parts = jnp.dot(
            spread[...], tiles[i].reshape(count * GROUP, keep), preferred_element_type=jnp.float32
        )
        value = (both_parts[:half] + both_parts[half:]).reshape(widths, GROUP, keep)
        part[d, t] = value
        return d, t, value

    for i in range(1, min(AHEAD, total)):
        load(i).start()

    ends_way = jnp.where(first, 0, 1)
    ends_peer = jnp.where(first, 1, n - 2)
    if late > 0:
        held = steps - jnp.where(first, HOLD_FIRST, HOLD_FINAL)
        kept = steps - jnp.where(first, KEEP_FIRST, KEEP_FINAL)
    else:
        held = steps

    @pl.when(end)
    def _():
        @pl.loop(0, total)
        def _(i):
            d, _, value = multiply(i)

            @pl.when(i == 0)
            def _():
                pl.semaphore_wait(barrier, 1 if n > 2 else peers)

            @pl.when(d != z)
            def _():
                pack(ends_way, i, value)

                @pl.when(i < held)
                def _():
                    launch(ends_way, i, ends_peer)

        if n == 2:
            to_peers(known)
            pl.semaphore_wait(known, peers - 1)

    def write(t):
        rows = pl.ds(pl.multiple_of(t * GROUP, GROUP), GROUP)
        return pltpu.make_async_copy(part.at[z, t], averages.at[:, rows, :], write_sem)

    def settle(t, value):
        part[z, t] = value
        write(t).start()

    def both_ways(t, value, second, counted):
        @pl.when(second)
        def _():
            settle(t, value)

            @pl.when(counted)
            def _():
                count_squares(value)

        @pl.when(jnp.logical_not(second))
        def _():
            part[z, t] = value

    up_delay = lag_up * (z - 1)
    down_delay = lag_down * (n - 2 - z)

    def pass_up(up):
        @pl.when(jnp.logical_and(up >= 0, up < (n - z) * groups))
        def _():
            d, t = upwards(up)
            value = part[d, t] + arrived(0, up)

            @pl.when(d == z)
            def _():
                s = turned(z, t, 1)
                second = z * groups + s + down_delay < up + up_delay
                both_ways(t, value, second, jnp.logical_or(z != 1, t < groups - late))

            extra = jnp.logical_and(z == n - 2, up < groups + late) if late > 0 else False

            @pl.when(jnp.logical_or(d != z, extra))
            def _():
                send(0, up, z + 1, value)

    def pass_down(down):
        @pl.when(jnp.logical_and(down >= 0, down < (z + 1) * groups))
        def _():
            d, t = downwards(down)
            value = part[d, t] + arrived(1, down)

            @pl.when(d == z)
            def _():
                s = turned(z, t, n - 2)
                second = (n - 1 - z) * groups + s + up_delay <= down + down_delay
                both_ways(t, value, second, jnp.logical_or(z != n - 2, t < groups - late))

            extra = jnp.logical_and(z == 1, down < groups + late) if late > 0 else False

            @pl.when(jnp.logical_or(d != z, extra))
            def _():
                send(1, down, z - 1, value)

    def pass_on(j):
        pass_up(j - up_delay)
        pass_down(j - down_delay)

    @pl.when(middle)
    def _():
        pl.loop(0, head)(lambda i: multiply(i) and None)
        pl.semaphore_wait(barrier, 2 + peers - 1)
        to_peers(known)

        @pl.loop(0, steps - late)
        def _(j):
            pass_on(j)

            for m in range(more):
                @pl.when(more * j + m + head < total)
                def _(m=m):
                    multiply(more * j + m + head)

            @pl.when(j == 2)
            def _():
                pl.semaphore_wait(known, peers - 1)

                @pl.when(z > 1)
                def _():
                    pl.semaphore_signal(token_down, inc=1, device_id={"snap": z - 1}, device_id_type=MESH)

                @pl.when(z < n - 2)
                def _():
                    pl.semaphore_signal(token_up, inc=1, device_id={"snap": z + 1}, device_id_type=MESH)

            @pl.when(j == 4)
            def _():
                @pl.when(z > 1)
                def _():
                    pl.semaphore_wait(token_up, 1)

                @pl.when(z < n - 2)
                def _():
                    pl.semaphore_wait(token_down, 1)

                @pl.when(z == 1)
                def _():
                    pl.semaphore_signal(complete, inc=1, device_id={"snap": z - 1}, device_id_type=MESH)

                @pl.when(z == n - 2)
                def _():
                    pl.semaphore_signal(complete, inc=1, device_id={"snap": z + 1}, device_id_type=MESH)

    if late > 0:
        @pl.when(z == 1)
        def _():
            pl.loop(steps - late - down_delay, 2 * groups)(pass_down)

        @pl.when(z == n - 2)
        def _():
            pl.loop(steps - late - up_delay, 2 * groups)(pass_up)

    @pl.when(end)
    def _():
        @pl.loop(0, groups + late)
        def _(k):
            if late > 0:
                early = k - (groups + late) + (kept - held)

                @pl.when(early >= 0)
                def _():
                    launch(ends_way, held + early, ends_peer)

            t = jnp.where(k < groups, k, 2 * groups - 1 - k)
            d = jnp.where(k < groups, z, ends_peer)
            value = part[d, t] + arrived(1 - ends_way, k)
            count_squares(value)

            @pl.when(k < groups)
            def _():
                settle(t, value)

        if n > 2:
            pl.semaphore_wait(complete, 1)

    sums = jnp.sum(jnp.sum(squares[...], axis=1), axis=1, keepdims=True)
    lanes = norms.shape[1]
    row = lax.broadcasted_iota(jnp.int32, (widths, lanes), 0)
    col = lax.broadcasted_iota(jnp.int32, (widths, lanes), 1)
    line = jnp.sum(jnp.where(row == col, sums, 0.0), axis=0, keepdims=True)

    mine = z * peers + me
    lines[mine] = line

    for p in range(n):
        def body(k, p=p):
            @pl.when(jnp.logical_or(p != z, k != me))
            def _():
                pltpu.make_async_remote_copy(
                    src_ref=lines.at[mine], dst_ref=lines.at[mine], send_sem=line_send, recv_sem=line_recv,
                    device_id={"snap": p, "param": k}, device_id_type=MESH,
                ).start()

        each(peers, body)

    if late > 0:
        @pl.when(end)
        def _():
            pl.loop(kept, steps)(lambda k: launch(ends_way, k, ends_peer))

        @pl.when(z == 1)
        def _():
            pl.loop(steps - late, steps - 1)(pass_up)

        @pl.when(z == n - 2)
        def _():
            pl.loop(steps - late, steps - 1)(pass_down)

    def sent(way, amount):
        if amount > 0:
            some = pl.ds(0, amount)
            pltpu.make_async_copy(out_code.at[way, some], out_code.at[way, some], send_sem.at[way]).wait()
            pltpu.make_async_copy(out_scale.at[way, some], out_scale.at[way, some], send_scale_sem.at[way]).wait()

    def all_sent(layers):
        for layer in layers:
            @pl.when(z == layer)
            def _(layer=layer):
                sent(0, (n - 1 - layer) * groups + (late if layer == n - 2 else 0))
                sent(1, layer * groups + (late if layer == 1 else 0))

    all_sent(range(1, n - 1))
    rest_of = lines.at[pl.ds(0, n * peers - 1)]
    pltpu.make_async_copy(rest_of, rest_of, line_send).wait()
    pltpu.make_async_copy(rest_of, rest_of, line_recv).wait()
    result[...] = jnp.sqrt(jnp.sum(lines[...], axis=0) / jnp.float32(entries))
    hand = pltpu.make_async_copy(result, norms, hand_sem)
    hand.start()

    if late > 0:
        @pl.when(z == 1)
        def _():
            pass_up(steps - 1)

        @pl.when(z == n - 2)
        def _():
            pass_down(steps - 1)

    all_sent((0, n - 1))
    pltpu.make_async_copy(averages, averages, write_sem).wait()
    hand.wait()


def hand_out(averages, norms, widths):
    def body(averages, norms, averages_out, norms_out, line, row, sems):
        parts = SPLIT
        size = averages.shape[0] // parts


        for k in range(parts):
            some = pl.ds(k * size, size)
            pltpu.make_async_copy(averages.at[some], averages_out.at[some], sems.at[k]).start()

        row[...] = norms[0, :widths]
        write = pltpu.make_async_copy(row, norms_out, sems.at[parts])
        write.start()
        for k in range(parts):
            some = pl.ds(k * size, size)
            pltpu.make_async_copy(averages.at[some], averages_out.at[some], sems.at[k]).wait()
        write.wait()

    anywhere = pl.BlockSpec(memory_space=pl.ANY)
    return pl.pallas_call(
        body,
        out_shape=(
            jax.ShapeDtypeStruct(averages.shape, jnp.float32),
            jax.ShapeDtypeStruct((widths,), jnp.float32),
        ),
        in_specs=[pl.BlockSpec(memory_space=pltpu.VMEM)] * 2,
        out_specs=(anywhere, anywhere),
        scratch_shapes=[pltpu.VMEM((1, 128), jnp.float32), pltpu.VMEM((widths,), jnp.float32), pltpu.SemaphoreType.DMA((SPLIT + 1,))],
        name="hand_out",
    )(pltpu.with_memory_space_constraint(averages, pltpu.VMEM), pltpu.with_memory_space_constraint(norms, pltpu.VMEM))


def on_device(n, peers, snapshots, coeffs):
    count, height, cols = snapshots.shape
    widths = coeffs.shape[0]
    keep = cols // n
    groups, steps, _, _ = shape_of(n, height)
    total = n * groups
    entries = height * cols * peers
    dma = pltpu.SemaphoreType.DMA
    regular = pltpu.SemaphoreType.REGULAR
    averages, norms = pl.pallas_call(
        functools.partial(kernel, n, peers, entries),
        out_shape=(
            jax.ShapeDtypeStruct((widths, height, keep), jnp.float32),
            jax.ShapeDtypeStruct((1, LANES), jnp.float32),
        ),
        in_specs=[pl.BlockSpec(memory_space=pl.ANY), pl.BlockSpec(memory_space=pl.ANY)],
        out_specs=(pl.BlockSpec(memory_space=pl.ANY), pl.BlockSpec(memory_space=pl.ANY)),
        scratch_shapes=[
            pltpu.VMEM((widths, count), jnp.float32),
            pltpu.VMEM((2 * widths * GROUP, count * GROUP), jnp.bfloat16),
            pltpu.VMEM((total, count, GROUP, keep), jnp.bfloat16),
            pltpu.VMEM((n, groups, widths, GROUP, keep), jnp.float32),
            pltpu.VMEM((2, steps, widths * GROUP, keep), jnp.bfloat16),
            pltpu.VMEM((2, steps, 1, LANES), jnp.float32),
            pltpu.VMEM((2, steps, widths * GROUP, keep), jnp.bfloat16),
            pltpu.VMEM((2, steps, 1, LANES), jnp.float32),
            pltpu.VMEM((widths, GROUP, LANES), jnp.float32),
            pltpu.VMEM((n * peers, 1, LANES), jnp.float32),
            pltpu.VMEM((1, LANES), jnp.float32),
            pltpu.VMEM((widths * GROUP // 2 * keep // LANES + 1, 1, LANES), jnp.float32),
            dma, dma((AHEAD + 1,)), dma, dma, dma((2,)), dma((2,)), dma((steps + max(2, n // 2) * groups,)), dma, dma,
            regular, regular, regular, regular,
        ],
        compiler_params=pltpu.CompilerParams(
            collective_id=0, has_side_effects=True, vmem_limit_bytes=48 * 1024 * 1024
        ),
        name="reconstruct",
    )(pltpu.with_memory_space_constraint(coeffs, pltpu.HBM), snapshots)
    return hand_out(averages, norms, widths)


def solution(mesh):
    in_specs = (P("snap", "param", None), P(None, "snap"))
    out_specs = (P(None, "param", "snap"), P())
    body = functools.partial(on_device, mesh.shape["snap"], mesh.shape["param"])
    return jax.shard_map(body, mesh=mesh, in_specs=in_specs, out_specs=out_specs, check_vma=False)
```

```python
import functools
import math

import jax
import jax.numpy as jnp
from jax import lax
from jax.experimental import pallas as pl
from jax.experimental.pallas import tpu as pltpu
from jax.sharding import PartitionSpec as P

MESH = pl.DeviceIdType.MESH
GROUP = 8
LAG_UP = 2
LAG_DOWN = 3
LATE = 6
HOLD_FIRST = (3, 3)
HOLD_FINAL = (4, 4)
BEHIND = 3
HEAD = 10
POWER = 15
AHEAD = 3
SPLIT = 1
SPLIT_FIRST = 1
TOP = 2.0**8.375
LANES = 128


def encode(value):
    lanes = [value[:, c:c + LANES] for c in range(0, value.shape[1], LANES)]
    largest = functools.reduce(jnp.maximum, [jnp.abs(lane) for lane in lanes])
    largest = jnp.maximum(jnp.max(largest, axis=0, keepdims=True), 1e-30)
    x = value * jnp.concatenate([TOP / largest] * len(lanes), axis=1)
    x2 = x * x
    x4 = x2 * x2
    x8 = x4 * x4
    return ((x8 * x4) * (x2 * x)).astype(jnp.bfloat16), largest * (1.0 / TOP)


def decode(code, scale):
    y = code.astype(jnp.float32)
    scale = jnp.concatenate([scale] * (code.shape[1] // LANES), axis=1)
    size = jnp.exp2(jnp.log2(jnp.maximum(jnp.abs(y), 1e-38)) * (1.0 / POWER)) * scale
    return jnp.where(y > 0.0, size, jnp.where(y < 0.0, -size, 0.0))


def each(size, body):
    if size <= 8:
        for k in range(size):
            body(k)
    else:
        pl.loop(0, size)(body)


def shape_of(n, height):
    groups = height // GROUP
    lags = min(LAG_UP, groups - 1), min(LAG_DOWN, groups - 1)
    late = min(LATE, groups - 1) if n > 3 else 0
    return groups, (n - 1) * groups, lags, late


def kernel(
    n, peers, entries, coeffs, stored, averages, norms,
    weights, spread, tiles, part, out_code, out_scale, in_code, in_scale, squares, lines, result, both_sizes,
    coeff_sem, load_sem, write_sem, hand_sem, send_sem, send_scale_sem, recv_sem, line_send, line_recv,
    known, token_up, token_down, complete,
):
    z = lax.axis_index("snap")
    me = lax.axis_index("param")
    widths, count = coeffs.shape
    keep = stored.shape[2] // n
    groups, steps, (lag_up, lag_down), late = shape_of(n, stored.shape[1])
    total = n * groups
    ring = load_sem.shape[0]
    low = z < n // 2
    first, final = z == 0, z == n - 1
    end = jnp.logical_or(first, final)
    middle = jnp.logical_not(end)
    hub = middle if n > 2 else end
    head = min(HEAD, total)
    more = 2

    def turned(d, s, last):
        return jnp.where(d == last, groups - 1 - s, s) if late > 0 else s

    def upwards(k):
        d = n - 1 - k // groups
        return d, turned(d, lax.rem(k, groups), n - 2)

    def downwards(k):
        d = k // groups
        return d, turned(d, lax.rem(k, groups), 1)

    def own(i):
        mixed = jnp.where(end, i, i // 2) if n % 2 == 0 else i
        rising = jnp.where(end, low, lax.rem(i, 2) == 0) if n % 2 == 0 else low
        du, tu = upwards(mixed)
        dd, td = downwards(mixed)
        return jnp.where(rising, du, dd), jnp.where(rising, tu, td)

    def load(i, begin=0, amount=count):
        d, t = own(i)
        some = pl.ds(begin, amount)
        return pltpu.make_async_copy(
            stored.at[some, pl.ds(pl.multiple_of(t * GROUP, GROUP), GROUP), pl.ds(pl.multiple_of(d * keep, keep), keep)],
            tiles.at[i, some],
            load_sem.at[lax.rem(i, ring)],
        )

    read = pltpu.make_async_copy(coeffs, weights, coeff_sem)
    read.start()
    split = math.gcd(SPLIT_FIRST, count)
    for c in range(split):
        load(0, c * (count // split), count // split).start()
    barrier = pltpu.get_barrier_semaphore()

    @pl.when(z > 0)
    def _():
        pl.semaphore_signal(barrier, inc=1, device_id={"snap": z - 1}, device_id_type=MESH)

    @pl.when(z < n - 1)
    def _():
        pl.semaphore_signal(barrier, inc=1, device_id={"snap": z + 1}, device_id_type=MESH)

    def to_peers(semaphore):
        def body(k):
            @pl.when(k != me)
            def _():
                pl.semaphore_signal(semaphore, inc=1, device_id={"param": k}, device_id_type=MESH)

        each(peers, body)

    @pl.when(hub)
    def _():
        to_peers(barrier)

    tall, wide = spread.shape
    row = lax.broadcasted_iota(jnp.int32, (count, wide), 0)
    col = lax.broadcasted_iota(jnp.int32, (count, wide), 1)
    repeat = jnp.where(col // GROUP == row, 1.0, 0.0).astype(jnp.bfloat16)
    row = lax.broadcasted_iota(jnp.int32, (GROUP, wide), 0)
    col = lax.broadcasted_iota(jnp.int32, (GROUP, wide), 1)
    same = (row == col % GROUP)[None]
    read.wait()
    whole = weights[...]
    high = whole.astype(jnp.bfloat16)
    rest = (whole - high.astype(jnp.float32)).astype(jnp.bfloat16)
    both = jnp.concatenate([high, rest], axis=0)
    full = jnp.dot(both, repeat, preferred_element_type=jnp.float32)
    full = jnp.where(same, full[:, None, :], 0.0)
    spread[...] = full.reshape(tall, wide).astype(jnp.bfloat16)
    squares[...] = jnp.zeros_like(squares)

    def place(layer, way, k):
        return jnp.where(jnp.where(layer < n // 2, 0, 1) == way, k, steps + k)

    def copies(way, k, peer):
        code = pltpu.make_async_remote_copy(
            src_ref=out_code.at[way, k], dst_ref=in_code.at[way, k],
            send_sem=send_sem.at[way], recv_sem=recv_sem.at[place(peer, way, k)],
            device_id={"snap": peer}, device_id_type=MESH,
        )
        scale = pltpu.make_async_remote_copy(
            src_ref=out_scale.at[way, k], dst_ref=in_scale.at[way, k],
            send_sem=send_scale_sem.at[way], recv_sem=recv_sem.at[place(peer, way, k)],
            device_id={"snap": peer}, device_id_type=MESH,
        )
        return scale, code

    def launch(way, k, peer):
        for copy in copies(way, k, peer):
            copy.start()

    def pack(way, k, value):
        code, scale = encode(value.reshape(widths * GROUP, keep))
        out_code[way, k] = code
        out_scale[way, k] = scale

    def send(way, k, peer, value):
        pack(way, k, value)
        launch(way, k, peer)

    def arrived(way, k):
        pltpu.make_async_copy(both_sizes, both_sizes, recv_sem.at[place(z, way, k)]).wait()
        return decode(in_code[way, k], in_scale[way, k]).reshape(widths, GROUP, keep)

    def count_squares(value):
        square = value * value
        squares[...] += sum(square[:, :, c:c + LANES] for c in range(0, keep, LANES))

    half = widths * GROUP

    def multiply(i):
        d, t = own(i)
        load(i).wait()

        @pl.when(i + AHEAD < total)
        def _():
            load(i + AHEAD).start()

        both_parts = jnp.dot(
            spread[...], tiles[i].reshape(count * GROUP, keep), preferred_element_type=jnp.float32
        )
        value = (both_parts[:half] + both_parts[half:]).reshape(widths, GROUP, keep)
        part[d, t] = value
        return d, t, value

    for i in range(1, min(AHEAD, total)):
        load(i).start()

    ends_way = jnp.where(first, 0, 1)
    ends_peer = jnp.where(first, 1, n - 2)
    if late > 0:
        second = lax.rem(me, 2) == 1
        held = steps - jnp.where(
            first, jnp.where(second, HOLD_FIRST[1], HOLD_FIRST[0]), jnp.where(second, HOLD_FINAL[1], HOLD_FINAL[0])
        )
    else:
        held = steps

    behind = jnp.where(lax.rem(me, 2) == 1, BEHIND, 0)

    @pl.when(end)
    def _():
        @pl.loop(0, total)
        def _(i):
            d, _, value = multiply(i)

            @pl.when(i == 0)
            def _():
                pl.semaphore_wait(barrier, 1 if n > 2 else peers)

            @pl.when(d != z)
            def _():
                pack(ends_way, i, value)

            ready = jnp.where(i == 0, 0, i - behind)

            @pl.when(jnp.logical_and(jnp.logical_or(i == 0, ready > 0), ready < held))
            def _():
                launch(ends_way, ready, ends_peer)

        if n == 2:
            to_peers(known)
            pl.semaphore_wait(known, peers - 1)

    def write(t):
        rows = pl.ds(pl.multiple_of(t * GROUP, GROUP), GROUP)
        return pltpu.make_async_copy(part.at[z, t], averages.at[:, rows, :], write_sem)

    def settle(t, value):
        part[z, t] = value
        write(t).start()

    def both_ways(t, value, second, counted):
        @pl.when(second)
        def _():
            settle(t, value)

            @pl.when(counted)
            def _():
                count_squares(value)

        @pl.when(jnp.logical_not(second))
        def _():
            part[z, t] = value

    up_delay = lag_up * (z - 1)
    down_delay = lag_down * (n - 2 - z)

    def pass_up(up):
        @pl.when(jnp.logical_and(up >= 0, up < (n - z) * groups))
        def _():
            d, t = upwards(up)
            value = part[d, t] + arrived(0, up)

            @pl.when(d == z)
            def _():
                s = turned(z, t, 1)
                second = z * groups + s + down_delay < up + up_delay
                both_ways(t, value, second, jnp.logical_or(z != 1, t < groups - late))

            extra = jnp.logical_and(z == n - 2, up < groups + late) if late > 0 else False

            @pl.when(jnp.logical_or(d != z, extra))
            def _():
                send(0, up, z + 1, value)

    def pass_down(down):
        @pl.when(jnp.logical_and(down >= 0, down < (z + 1) * groups))
        def _():
            d, t = downwards(down)
            value = part[d, t] + arrived(1, down)

            @pl.when(d == z)
            def _():
                s = turned(z, t, n - 2)
                second = (n - 1 - z) * groups + s + up_delay <= down + down_delay
                both_ways(t, value, second, jnp.logical_or(z != n - 2, t < groups - late))

            extra = jnp.logical_and(z == 1, down < groups + late) if late > 0 else False

            @pl.when(jnp.logical_or(d != z, extra))
            def _():
                send(1, down, z - 1, value)

    def pass_on(j):
        pass_up(j - up_delay)
        pass_down(j - down_delay)

    @pl.when(middle)
    def _():
        pl.loop(0, head)(lambda i: multiply(i) and None)
        pl.semaphore_wait(barrier, 2 + peers - 1)
        to_peers(known)

        @pl.loop(0, steps - late)
        def _(j):
            pass_on(j)

            for m in range(more):
                @pl.when(more * j + m + head < total)
                def _(m=m):
                    multiply(more * j + m + head)

            @pl.when(j == 2)
            def _():
                pl.semaphore_wait(known, peers - 1)

                @pl.when(jnp.logical_and(z == n - 2, z > 1))
                def _():
                    pl.semaphore_signal(token_down, inc=1, device_id={"snap": z - 1}, device_id_type=MESH)

                @pl.when(jnp.logical_and(z == 1, z < n - 2))
                def _():
                    pl.semaphore_signal(token_up, inc=1, device_id={"snap": z + 1}, device_id_type=MESH)

            @pl.when(j == 4)
            def _():
                @pl.when(z > 1)
                def _():
                    pl.semaphore_wait(token_up, 1)

                @pl.when(jnp.logical_and(z > 1, z < n - 2))
                def _():
                    pl.semaphore_signal(token_up, inc=1, device_id={"snap": z + 1}, device_id_type=MESH)

                @pl.when(z < n - 2)
                def _():
                    pl.semaphore_wait(token_down, 1)

                @pl.when(jnp.logical_and(z > 1, z < n - 2))
                def _():
                    pl.semaphore_signal(token_down, inc=1, device_id={"snap": z - 1}, device_id_type=MESH)

                @pl.when(z == 1)
                def _():
                    pl.semaphore_signal(complete, inc=1, device_id={"snap": z - 1}, device_id_type=MESH)

                @pl.when(z == n - 2)
                def _():
                    pl.semaphore_signal(complete, inc=1, device_id={"snap": z + 1}, device_id_type=MESH)

    if late > 0:
        @pl.when(z == 1)
        def _():
            pl.loop(steps - late - down_delay, 2 * groups)(pass_down)

        @pl.when(z == n - 2)
        def _():
            pl.loop(steps - late - up_delay, 2 * groups)(pass_up)

    @pl.when(end)
    def _():
        @pl.loop(0, groups + late)
        def _(k):
            t = jnp.where(k < groups, k, 2 * groups - 1 - k)
            d = jnp.where(k < groups, z, ends_peer)
            value = part[d, t] + arrived(1 - ends_way, k)
            count_squares(value)

            @pl.when(k < groups)
            def _():
                settle(t, value)

        if n > 2:
            pl.semaphore_wait(complete, 1)

    sums = jnp.sum(jnp.sum(squares[...], axis=1), axis=1, keepdims=True)
    lanes = norms.shape[1]
    row = lax.broadcasted_iota(jnp.int32, (widths, lanes), 0)
    col = lax.broadcasted_iota(jnp.int32, (widths, lanes), 1)
    line = jnp.sum(jnp.where(row == col, sums, 0.0), axis=0, keepdims=True)

    mine = z * peers + me
    lines[mine] = line

    for p in range(n):
        def body(k, p=p):
            @pl.when(jnp.logical_or(p != z, k != me))
            def _():
                pltpu.make_async_remote_copy(
                    src_ref=lines.at[mine], dst_ref=lines.at[mine], send_sem=line_send, recv_sem=line_recv,
                    device_id={"snap": p, "param": k}, device_id_type=MESH,
                ).start()

        each(peers, body)

    if late > 0:
        @pl.when(end)
        def _():
            pl.loop(held, steps)(lambda k: launch(ends_way, k, ends_peer))

        @pl.when(z == 1)
        def _():
            pl.loop(steps - late, steps - 1)(pass_up)

        @pl.when(z == n - 2)
        def _():
            pl.loop(steps - late, steps - 1)(pass_down)

    def sent(way, amount):
        if amount > 0:
            some = pl.ds(0, amount)
            pltpu.make_async_copy(out_code.at[way, some], out_code.at[way, some], send_sem.at[way]).wait()
            pltpu.make_async_copy(out_scale.at[way, some], out_scale.at[way, some], send_scale_sem.at[way]).wait()

    def all_sent(layers):
        for layer in layers:
            @pl.when(z == layer)
            def _(layer=layer):
                sent(0, (n - 1 - layer) * groups + (late if layer == n - 2 else 0))
                sent(1, layer * groups + (late if layer == 1 else 0))

    all_sent(range(1, n - 1))
    rest_of = lines.at[pl.ds(0, n * peers - 1)]
    pltpu.make_async_copy(rest_of, rest_of, line_send).wait()
    pltpu.make_async_copy(rest_of, rest_of, line_recv).wait()
    result[...] = jnp.sqrt(jnp.sum(lines[...], axis=0) / jnp.float32(entries))
    hand = pltpu.make_async_copy(result, norms, hand_sem)
    hand.start()

    if late > 0:
        @pl.when(z == 1)
        def _():
            pass_up(steps - 1)

        @pl.when(z == n - 2)
        def _():
            pass_down(steps - 1)

    all_sent((0, n - 1))
    pltpu.make_async_copy(averages, averages, write_sem).wait()
    hand.wait()


def hand_out(averages, norms, widths):
    def body(averages, norms, averages_out, norms_out, line, row, sems):
        parts = SPLIT
        size = averages.shape[0] // parts


        for k in range(parts):
            some = pl.ds(k * size, size)
            pltpu.make_async_copy(averages.at[some], averages_out.at[some], sems.at[k]).start()

        row[...] = norms[0, :widths]
        write = pltpu.make_async_copy(row, norms_out, sems.at[parts])
        write.start()
        for k in range(parts):
            some = pl.ds(k * size, size)
            pltpu.make_async_copy(averages.at[some], averages_out.at[some], sems.at[k]).wait()
        write.wait()

    anywhere = pl.BlockSpec(memory_space=pl.ANY)
    return pl.pallas_call(
        body,
        out_shape=(
            jax.ShapeDtypeStruct(averages.shape, jnp.float32),
            jax.ShapeDtypeStruct((widths,), jnp.float32),
        ),
        in_specs=[pl.BlockSpec(memory_space=pltpu.VMEM)] * 2,
        out_specs=(anywhere, anywhere),
        scratch_shapes=[pltpu.VMEM((1, 128), jnp.float32), pltpu.VMEM((widths,), jnp.float32), pltpu.SemaphoreType.DMA((SPLIT + 1,))],
        name="hand_out",
    )(pltpu.with_memory_space_constraint(averages, pltpu.VMEM), pltpu.with_memory_space_constraint(norms, pltpu.VMEM))


def on_device(n, peers, snapshots, coeffs):
    count, height, cols = snapshots.shape
    widths = coeffs.shape[0]
    keep = cols // n
    groups, steps, _, _ = shape_of(n, height)
    total = n * groups
    entries = height * cols * peers
    dma = pltpu.SemaphoreType.DMA
    regular = pltpu.SemaphoreType.REGULAR
    averages, norms = pl.pallas_call(
        functools.partial(kernel, n, peers, entries),
        out_shape=(
            jax.ShapeDtypeStruct((widths, height, keep), jnp.float32),
            jax.ShapeDtypeStruct((1, LANES), jnp.float32),
        ),
        in_specs=[pl.BlockSpec(memory_space=pl.ANY), pl.BlockSpec(memory_space=pl.ANY)],
        out_specs=(pl.BlockSpec(memory_space=pl.ANY), pl.BlockSpec(memory_space=pl.ANY)),
        scratch_shapes=[
            pltpu.VMEM((widths, count), jnp.float32),
            pltpu.VMEM((2 * widths * GROUP, count * GROUP), jnp.bfloat16),
            pltpu.VMEM((total, count, GROUP, keep), jnp.bfloat16),
            pltpu.VMEM((n, groups, widths, GROUP, keep), jnp.float32),
            pltpu.VMEM((2, steps, widths * GROUP, keep), jnp.bfloat16),
            pltpu.VMEM((2, steps, 1, LANES), jnp.float32),
            pltpu.VMEM((2, steps, widths * GROUP, keep), jnp.bfloat16),
            pltpu.VMEM((2, steps, 1, LANES), jnp.float32),
            pltpu.VMEM((widths, GROUP, LANES), jnp.float32),
            pltpu.VMEM((n * peers, 1, LANES), jnp.float32),
            pltpu.VMEM((1, LANES), jnp.float32),
            pltpu.VMEM((widths * GROUP // 2 * keep // LANES + 1, 1, LANES), jnp.float32),
            dma, dma((AHEAD + 1,)), dma, dma, dma((2,)), dma((2,)), dma((steps + max(2, n // 2) * groups,)), dma, dma,
            regular, regular, regular, regular,
        ],
        compiler_params=pltpu.CompilerParams(
            collective_id=0, has_side_effects=True, vmem_limit_bytes=48 * 1024 * 1024
        ),
        name="reconstruct",
    )(pltpu.with_memory_space_constraint(coeffs, pltpu.HBM), snapshots)
    return hand_out(averages, norms, widths)


def solution(mesh):
    in_specs = (P("snap", "param", None), P(None, "snap"))
    out_specs = (P(None, "param", "snap"), P())
    body = functools.partial(on_device, mesh.shape["snap"], mesh.shape["param"])
    return jax.shard_map(body, mesh=mesh, in_specs=in_specs, out_specs=out_specs, check_vma=False)
```

```python
import functools
import math

import jax
import jax.numpy as jnp
from jax import lax
from jax.experimental import pallas as pl
from jax.experimental.pallas import tpu as pltpu
from jax.sharding import PartitionSpec as P

MESH = pl.DeviceIdType.MESH
GROUP = 8
LAG_UP = 2
LAG_DOWN = 3
LATE = 6
HOLD_FIRST = (3, 3)
HOLD_FINAL = (4, 4)
BEHIND = (5, 3)
HEAD = 10
POWER = 15
AHEAD = 3
SPLIT = 1
SPLIT_FIRST = 1
TOP = 2.0**8.375
LANES = 128


def encode(value):
    lanes = [value[:, c:c + LANES] for c in range(0, value.shape[1], LANES)]
    largest = functools.reduce(jnp.maximum, [jnp.abs(lane) for lane in lanes])
    largest = jnp.maximum(jnp.max(largest, axis=0, keepdims=True), 1e-30)
    x = value * jnp.concatenate([TOP / largest] * len(lanes), axis=1)
    x2 = x * x
    x4 = x2 * x2
    x8 = x4 * x4
    return ((x8 * x4) * (x2 * x)).astype(jnp.bfloat16), largest * (1.0 / TOP)


def decode(code, scale):
    y = code.astype(jnp.float32)
    scale = jnp.concatenate([scale] * (code.shape[1] // LANES), axis=1)
    size = jnp.exp2(jnp.log2(jnp.maximum(jnp.abs(y), 1e-38)) * (1.0 / POWER)) * scale
    return jnp.where(y > 0.0, size, jnp.where(y < 0.0, -size, 0.0))


def each(size, body):
    if size <= 8:
        for k in range(size):
            body(k)
    else:
        pl.loop(0, size)(body)


def shape_of(n, height):
    groups = height // GROUP
    lags = min(LAG_UP, groups - 1), min(LAG_DOWN, groups - 1)
    late = min(LATE, groups - 1) if n > 3 else 0
    return groups, (n - 1) * groups, lags, late


def kernel(
    n, peers, entries, coeffs, stored, averages, norms,
    weights, spread, tiles, part, out_code, out_scale, in_code, in_scale, squares, lines, result, sizes,
    coeff_sem, load_sem, write_sem, send_sem, recv_sem, line_recv,
    known, token_up, token_down, complete,
):
    z = lax.axis_index("snap")
    me = lax.axis_index("param")
    widths, count = coeffs.shape
    keep = stored.shape[2] // n
    groups, steps, (lag_up, lag_down), late = shape_of(n, stored.shape[1])
    total = n * groups
    ring = load_sem.shape[0]
    low = z < n // 2
    first, final = z == 0, z == n - 1
    end = jnp.logical_or(first, final)
    middle = jnp.logical_not(end)
    hub = middle if n > 2 else end
    head = min(HEAD, total)
    more = 2

    def turned(d, s, last):
        return jnp.where(d == last, groups - 1 - s, s) if late > 0 else s

    def upwards(k):
        d = n - 1 - k // groups
        return d, turned(d, lax.rem(k, groups), n - 2)

    def downwards(k):
        d = k // groups
        return d, turned(d, lax.rem(k, groups), 1)

    def own(i):
        mixed = jnp.where(end, i, i // 2) if n % 2 == 0 else i
        rising = jnp.where(end, low, lax.rem(i, 2) == 0) if n % 2 == 0 else low
        du, tu = upwards(mixed)
        dd, td = downwards(mixed)
        return jnp.where(rising, du, dd), jnp.where(rising, tu, td)

    def load(i, begin=0, amount=count):
        d, t = own(i)
        some = pl.ds(begin, amount)
        return pltpu.make_async_copy(
            stored.at[some, pl.ds(pl.multiple_of(t * GROUP, GROUP), GROUP), pl.ds(pl.multiple_of(d * keep, keep), keep)],
            tiles.at[i, some],
            load_sem.at[lax.rem(i, ring)],
        )

    read = pltpu.make_async_copy(coeffs, weights, coeff_sem)
    read.start()
    split = math.gcd(SPLIT_FIRST, count)
    for c in range(split):
        load(0, c * (count // split), count // split).start()
    barrier = pltpu.get_barrier_semaphore()

    @pl.when(z > 0)
    def _():
        pl.semaphore_signal(barrier, inc=1, device_id={"snap": z - 1}, device_id_type=MESH)

    @pl.when(z < n - 1)
    def _():
        pl.semaphore_signal(barrier, inc=1, device_id={"snap": z + 1}, device_id_type=MESH)

    def to_peers(semaphore):
        def body(k):
            @pl.when(k != me)
            def _():
                pl.semaphore_signal(semaphore, inc=1, device_id={"param": k}, device_id_type=MESH)

        each(peers, body)

    @pl.when(hub)
    def _():
        to_peers(barrier)

    tall, wide = spread.shape
    row = lax.broadcasted_iota(jnp.int32, (count, wide), 0)
    col = lax.broadcasted_iota(jnp.int32, (count, wide), 1)
    repeat = jnp.where(col // GROUP == row, 1.0, 0.0).astype(jnp.bfloat16)
    row = lax.broadcasted_iota(jnp.int32, (GROUP, wide), 0)
    col = lax.broadcasted_iota(jnp.int32, (GROUP, wide), 1)
    same = (row == col % GROUP)[None]
    read.wait()
    whole = weights[...]
    high = whole.astype(jnp.bfloat16)
    rest = (whole - high.astype(jnp.float32)).astype(jnp.bfloat16)
    both = jnp.concatenate([high, rest], axis=0)
    full = jnp.dot(both, repeat, preferred_element_type=jnp.float32)
    full = jnp.where(same, full[:, None, :], 0.0)
    spread[...] = full.reshape(tall, wide).astype(jnp.bfloat16)
    squares[...] = jnp.zeros_like(squares)

    def place(layer, way, k):
        return jnp.where(jnp.where(layer < n // 2, 0, 1) == way, k, steps + k)

    def copies(way, k, peer):
        code = pltpu.make_async_remote_copy(
            src_ref=out_code.at[way, k], dst_ref=in_code.at[way, k],
            send_sem=send_sem, recv_sem=recv_sem.at[place(peer, way, k)],
            device_id={"snap": peer}, device_id_type=MESH,
        )
        scale = pltpu.make_async_remote_copy(
            src_ref=out_scale.at[way, k], dst_ref=in_scale.at[way, k],
            send_sem=send_sem, recv_sem=recv_sem.at[place(peer, way, k)],
            device_id={"snap": peer}, device_id_type=MESH,
        )
        return scale, code

    def launch(way, k, peer):
        for copy in copies(way, k, peer):
            copy.start()

    def pack(way, k, value):
        code, scale = encode(value.reshape(widths * GROUP, keep))
        out_code[way, k] = code
        out_scale[way, k] = scale

    def send(way, k, peer, value):
        pack(way, k, value)
        launch(way, k, peer)

    chunk = widths * GROUP // 2 * keep // LANES + 1

    def await_sizes(chunks, more_lines, semaphore):
        some = sizes.at[pl.ds(0, chunks * chunk + more_lines)]
        pltpu.make_async_copy(some, some, semaphore).wait()

    def arrived(way, k):
        await_sizes(1, 0, recv_sem.at[place(z, way, k)])
        return decode(in_code[way, k], in_scale[way, k]).reshape(widths, GROUP, keep)

    def count_squares(value):
        square = value * value
        squares[...] += sum(square[:, :, c:c + LANES] for c in range(0, keep, LANES))

    half = widths * GROUP

    def multiply(i):
        d, t = own(i)
        load(i).wait()

        @pl.when(i + AHEAD < total)
        def _():
            load(i + AHEAD).start()

        both_parts = jnp.dot(
            spread[...], tiles[i].reshape(count * GROUP, keep), preferred_element_type=jnp.float32
        )
        value = (both_parts[:half] + both_parts[half:]).reshape(widths, GROUP, keep)
        part[d, t] = value
        return d, t, value

    for i in range(1, min(AHEAD, total)):
        load(i).start()

    ends_way = jnp.where(first, 0, 1)
    ends_peer = jnp.where(first, 1, n - 2)
    if late > 0:
        second = lax.rem(me, 2) == 1
        held = steps - jnp.where(
            first, jnp.where(second, HOLD_FIRST[1], HOLD_FIRST[0]), jnp.where(second, HOLD_FINAL[1], HOLD_FINAL[0])
        )
    else:
        held = steps

    behind = jnp.where(lax.rem(me, 2) == 1, jnp.where(first, BEHIND[0], BEHIND[1]), 0)

    @pl.when(end)
    def _():
        @pl.loop(0, total)
        def _(i):
            d, _, value = multiply(i)

            @pl.when(i == 0)
            def _():
                pl.semaphore_wait(barrier, 1 if n > 2 else peers)

            @pl.when(d != z)
            def _():
                pack(ends_way, i, value)

            ready = jnp.where(i == 0, 0, i - behind)

            @pl.when(jnp.logical_and(jnp.logical_or(i == 0, ready > 0), ready < held))
            def _():
                launch(ends_way, ready, ends_peer)

        if n == 2:
            to_peers(known)
            pl.semaphore_wait(known, peers - 1)

    def write(t):
        rows = pl.ds(pl.multiple_of(t * GROUP, GROUP), GROUP)
        return pltpu.make_async_copy(part.at[z, t], averages.at[:, rows, :], write_sem)

    def settle(t, value):
        part[z, t] = value
        write(t).start()

    def both_ways(t, value, second, counted):
        @pl.when(second)
        def _():
            settle(t, value)

            @pl.when(counted)
            def _():
                count_squares(value)

        @pl.when(jnp.logical_not(second))
        def _():
            part[z, t] = value

    up_delay = lag_up * (z - 1)
    down_delay = lag_down * (n - 2 - z)

    def pass_up(up):
        @pl.when(jnp.logical_and(up >= 0, up < (n - z) * groups))
        def _():
            d, t = upwards(up)
            value = part[d, t] + arrived(0, up)

            @pl.when(d == z)
            def _():
                s = turned(z, t, 1)
                second = z * groups + s + down_delay < up + up_delay
                both_ways(t, value, second, jnp.logical_or(z != 1, t < groups - late))

            extra = jnp.logical_and(z == n - 2, up < groups + late) if late > 0 else False

            @pl.when(jnp.logical_or(d != z, extra))
            def _():
                send(0, up, z + 1, value)

    def pass_down(down):
        @pl.when(jnp.logical_and(down >= 0, down < (z + 1) * groups))
        def _():
            d, t = downwards(down)
            value = part[d, t] + arrived(1, down)

            @pl.when(d == z)
            def _():
                s = turned(z, t, n - 2)
                second = (n - 1 - z) * groups + s + up_delay <= down + down_delay
                both_ways(t, value, second, jnp.logical_or(z != n - 2, t < groups - late))

            extra = jnp.logical_and(z == 1, down < groups + late) if late > 0 else False

            @pl.when(jnp.logical_or(d != z, extra))
            def _():
                send(1, down, z - 1, value)

    def pass_on(j):
        pass_up(j - up_delay)
        pass_down(j - down_delay)

    @pl.when(middle)
    def _():
        pl.loop(0, head)(lambda i: multiply(i) and None)
        pl.semaphore_wait(barrier, 2 + peers - 1)
        to_peers(known)

        @pl.loop(0, steps - late)
        def _(j):
            pass_on(j)

            for m in range(more):
                @pl.when(more * j + m + head < total)
                def _(m=m):
                    multiply(more * j + m + head)

            @pl.when(j == 2)
            def _():
                pl.semaphore_wait(known, peers - 1)

                @pl.when(jnp.logical_and(z == n - 2, z > 1))
                def _():
                    pl.semaphore_signal(token_down, inc=1, device_id={"snap": z - 1}, device_id_type=MESH)

                @pl.when(jnp.logical_and(z == 1, z < n - 2))
                def _():
                    pl.semaphore_signal(token_up, inc=1, device_id={"snap": z + 1}, device_id_type=MESH)

            @pl.when(j == 4)
            def _():
                @pl.when(z > 1)
                def _():
                    pl.semaphore_wait(token_up, 1)

                @pl.when(jnp.logical_and(z > 1, z < n - 2))
                def _():
                    pl.semaphore_signal(token_up, inc=1, device_id={"snap": z + 1}, device_id_type=MESH)

                @pl.when(z < n - 2)
                def _():
                    pl.semaphore_wait(token_down, 1)

                @pl.when(jnp.logical_and(z > 1, z < n - 2))
                def _():
                    pl.semaphore_signal(token_down, inc=1, device_id={"snap": z - 1}, device_id_type=MESH)

                @pl.when(z == 1)
                def _():
                    pl.semaphore_signal(complete, inc=1, device_id={"snap": z - 1}, device_id_type=MESH)

                @pl.when(z == n - 2)
                def _():
                    pl.semaphore_signal(complete, inc=1, device_id={"snap": z + 1}, device_id_type=MESH)

    if late > 0:
        @pl.when(z == 1)
        def _():
            pl.loop(steps - late - down_delay, 2 * groups)(pass_down)

        @pl.when(z == n - 2)
        def _():
            pl.loop(steps - late - up_delay, 2 * groups)(pass_up)

    @pl.when(end)
    def _():
        @pl.loop(0, groups + late)
        def _(k):
            t = jnp.where(k < groups, k, 2 * groups - 1 - k)
            d = jnp.where(k < groups, z, ends_peer)
            value = part[d, t] + arrived(1 - ends_way, k)
            count_squares(value)

            @pl.when(k < groups)
            def _():
                settle(t, value)

        if n > 2:
            pl.semaphore_wait(complete, 1)

    sums = jnp.sum(jnp.sum(squares[...], axis=1), axis=1, keepdims=True)
    lanes = norms.shape[1]
    row = lax.broadcasted_iota(jnp.int32, (widths, lanes), 0)
    col = lax.broadcasted_iota(jnp.int32, (widths, lanes), 1)
    line = jnp.sum(jnp.where(row == col, sums, 0.0), axis=0, keepdims=True)

    mine = z * peers + me
    lines[mine] = line

    for p in range(n):
        def body(k, p=p):
            @pl.when(jnp.logical_or(p != z, k != me))
            def _():
                pltpu.make_async_remote_copy(
                    src_ref=lines.at[mine], dst_ref=lines.at[mine], send_sem=send_sem, recv_sem=line_recv,
                    device_id={"snap": p, "param": k}, device_id_type=MESH,
                ).start()

        each(peers, body)

    if late > 0:
        @pl.when(end)
        def _():
            pl.loop(held, steps)(lambda k: launch(ends_way, k, ends_peer))

        @pl.when(z == 1)
        def _():
            pl.loop(steps - late, steps - 1)(pass_up)

        @pl.when(z == n - 2)
        def _():
            pl.loop(steps - late, steps - 1)(pass_down)

    def all_sent(layers):
        for layer in layers:
            @pl.when(z == layer)
            def _(layer=layer):
                extra = late * (layer == n - 2) + late * (layer == 1)
                await_sizes((n - 1) * groups + extra, n * peers - 1, send_sem)

    all_sent(range(1, n - 1))
    await_sizes(0, n * peers - 1, line_recv)
    result[...] = jnp.sqrt(jnp.sum(lines[...], axis=0) / jnp.float32(entries))
    hand = pltpu.make_async_copy(result, norms, coeff_sem)
    hand.start()

    if late > 0:
        @pl.when(z == 1)
        def _():
            pass_up(steps - 1)

        @pl.when(z == n - 2)
        def _():
            pass_down(steps - 1)

    all_sent((0, n - 1))
    pltpu.make_async_copy(averages, averages, write_sem).wait()
    hand.wait()


def hand_out(averages, norms, widths):
    def body(averages, norms, averages_out, norms_out, line, row, sems):
        parts = SPLIT
        size = averages.shape[0] // parts


        for k in range(parts):
            some = pl.ds(k * size, size)
            pltpu.make_async_copy(averages.at[some], averages_out.at[some], sems.at[k]).start()

        row[...] = norms[0, :widths]
        write = pltpu.make_async_copy(row, norms_out, sems.at[parts])
        write.start()
        for k in range(parts):
            some = pl.ds(k * size, size)
            pltpu.make_async_copy(averages.at[some], averages_out.at[some], sems.at[k]).wait()
        write.wait()

    anywhere = pl.BlockSpec(memory_space=pl.ANY)
    return pl.pallas_call(
        body,
        out_shape=(
            jax.ShapeDtypeStruct(averages.shape, jnp.float32),
            jax.ShapeDtypeStruct((widths,), jnp.float32),
        ),
        in_specs=[pl.BlockSpec(memory_space=pltpu.VMEM)] * 2,
        out_specs=(anywhere, anywhere),
        scratch_shapes=[pltpu.VMEM((1, 128), jnp.float32), pltpu.VMEM((widths,), jnp.float32), pltpu.SemaphoreType.DMA((SPLIT + 1,))],
        name="hand_out",
    )(pltpu.with_memory_space_constraint(averages, pltpu.VMEM), pltpu.with_memory_space_constraint(norms, pltpu.VMEM))


def on_device(n, peers, snapshots, coeffs):
    count, height, cols = snapshots.shape
    widths = coeffs.shape[0]
    keep = cols // n
    groups, steps, _, _ = shape_of(n, height)
    total = n * groups
    entries = height * cols * peers
    dma = pltpu.SemaphoreType.DMA
    regular = pltpu.SemaphoreType.REGULAR
    averages, norms = pl.pallas_call(
        functools.partial(kernel, n, peers, entries),
        out_shape=(
            jax.ShapeDtypeStruct((widths, height, keep), jnp.float32),
            jax.ShapeDtypeStruct((1, LANES), jnp.float32),
        ),
        in_specs=[pl.BlockSpec(memory_space=pl.ANY), pl.BlockSpec(memory_space=pl.ANY)],
        out_specs=(pl.BlockSpec(memory_space=pl.ANY), pl.BlockSpec(memory_space=pl.ANY)),
        scratch_shapes=[
            pltpu.VMEM((widths, count), jnp.float32),
            pltpu.VMEM((2 * widths * GROUP, count * GROUP), jnp.bfloat16),
            pltpu.VMEM((total, count, GROUP, keep), jnp.bfloat16),
            pltpu.VMEM((n, groups, widths, GROUP, keep), jnp.float32),
            pltpu.VMEM((2, steps, widths * GROUP, keep), jnp.bfloat16),
            pltpu.VMEM((2, steps, 1, LANES), jnp.float32),
            pltpu.VMEM((2, steps, widths * GROUP, keep), jnp.bfloat16),
            pltpu.VMEM((2, steps, 1, LANES), jnp.float32),
            pltpu.VMEM((widths, GROUP, LANES), jnp.float32),
            pltpu.VMEM((n * peers, 1, LANES), jnp.float32),
            pltpu.VMEM((1, LANES), jnp.float32),
            pltpu.VMEM((2 * steps * (widths * GROUP // 2 * keep // LANES + 1) + n * peers, 1, LANES), jnp.float32),
            dma, dma((AHEAD + 1,)), dma, dma, dma((steps + max(2, n // 2) * groups,)), dma,
            regular, regular, regular, regular,
        ],
        compiler_params=pltpu.CompilerParams(
            collective_id=0, has_side_effects=True, vmem_limit_bytes=48 * 1024 * 1024
        ),
        name="reconstruct",
    )(pltpu.with_memory_space_constraint(coeffs, pltpu.HBM), snapshots)
    return hand_out(averages, norms, widths)


def solution(mesh):
    in_specs = (P("snap", "param", None), P(None, "snap"))
    out_specs = (P(None, "param", "snap"), P())
    body = functools.partial(on_device, mesh.shape["snap"], mesh.shape["param"])
    return jax.shard_map(body, mesh=mesh, in_specs=in_specs, out_specs=out_specs, check_vma=False)
```

```python
import functools
import math

import jax
import jax.numpy as jnp
from jax import lax
from jax.experimental import pallas as pl
from jax.experimental.pallas import tpu as pltpu
from jax.sharding import PartitionSpec as P

MESH = pl.DeviceIdType.MESH
GROUP = 8
LAG_UP = 2
LAG_DOWN = 3
LATE = 6
HOLD_FIRST = (3, 3)
HOLD_FINAL = (4, 4)
BEHIND = (5, 3)
HEAD = 10
POWER = 15
AHEAD = 3
SPLIT = 1
SPLIT_FIRST = 1
TOP = 2.0**8.375
LANES = 128


def encode(value):
    lanes = [value[:, c:c + LANES] for c in range(0, value.shape[1], LANES)]
    largest = functools.reduce(jnp.maximum, [jnp.abs(lane) for lane in lanes])
    largest = jnp.maximum(jnp.max(largest, axis=0, keepdims=True), 1e-30)
    x = value * jnp.concatenate([TOP / largest] * len(lanes), axis=1)
    x2 = x * x
    x4 = x2 * x2
    x8 = x4 * x4
    return ((x8 * x4) * (x2 * x)).astype(jnp.bfloat16), largest * (1.0 / TOP)


def decode(code, scale):
    y = code.astype(jnp.float32)
    scale = jnp.concatenate([scale] * (code.shape[1] // LANES), axis=1)
    size = jnp.exp2(jnp.log2(jnp.maximum(jnp.abs(y), 1e-38)) * (1.0 / POWER)) * scale
    return jnp.where(y > 0.0, size, jnp.where(y < 0.0, -size, 0.0))


def each(size, body):
    if size <= 8:
        for k in range(size):
            body(k)
    else:
        pl.loop(0, size)(body)


def shape_of(n, height):
    groups = height // GROUP
    lags = min(LAG_UP, groups - 1), min(LAG_DOWN, groups - 1)
    late = min(LATE, groups - 1) if n > 3 else 0
    return groups, (n - 1) * groups, lags, late


def kernel(
    n, peers, entries, coeffs, stored, averages, norms,
    weights, spread, tiles, part, out_code, out_scale, in_code, in_scale, squares, lines, result, sizes,
    coeff_sem, load_sem, write_sem, send_sem, recv_sem, line_recv,
    known, token_up, token_down, complete,
):
    z = lax.axis_index("snap")
    me = lax.axis_index("param")
    widths, count = coeffs.shape
    keep = stored.shape[2] // n
    groups, steps, (lag_up, lag_down), late = shape_of(n, stored.shape[1])
    total = n * groups
    ring = load_sem.shape[0]
    low = z < n // 2
    first, final = z == 0, z == n - 1
    end = jnp.logical_or(first, final)
    middle = jnp.logical_not(end)
    hub = middle if n > 2 else end
    head = min(HEAD, total)
    more = 2

    def turned(d, s, last):
        return jnp.where(d == last, groups - 1 - s, s) if late > 0 else s

    def upwards(k):
        d = n - 1 - k // groups
        return d, turned(d, lax.rem(k, groups), n - 2)

    def downwards(k):
        d = k // groups
        return d, turned(d, lax.rem(k, groups), 1)

    def own(i):
        mixed = jnp.where(end, i, i // 2) if n % 2 == 0 else i
        rising = jnp.where(end, low, lax.rem(i, 2) == 0) if n % 2 == 0 else low
        du, tu = upwards(mixed)
        dd, td = downwards(mixed)
        return jnp.where(rising, du, dd), jnp.where(rising, tu, td)

    def load(i, begin=0, amount=count):
        d, t = own(i)
        some = pl.ds(begin, amount)
        return pltpu.make_async_copy(
            stored.at[some, pl.ds(pl.multiple_of(t * GROUP, GROUP), GROUP), pl.ds(pl.multiple_of(d * keep, keep), keep)],
            tiles.at[i, some],
            load_sem.at[lax.rem(i, ring)],
        )

    read = pltpu.make_async_copy(coeffs, weights, coeff_sem)
    read.start()
    split = math.gcd(SPLIT_FIRST, count)
    for c in range(split):
        load(0, c * (count // split), count // split).start()
    barrier = pltpu.get_barrier_semaphore()

    @pl.when(z > 0)
    def _():
        pl.semaphore_signal(barrier, inc=1, device_id={"snap": z - 1}, device_id_type=MESH)

    @pl.when(z < n - 1)
    def _():
        pl.semaphore_signal(barrier, inc=1, device_id={"snap": z + 1}, device_id_type=MESH)

    def to_peers(semaphore):
        def body(k):
            @pl.when(k != me)
            def _():
                pl.semaphore_signal(semaphore, inc=1, device_id={"param": k}, device_id_type=MESH)

        each(peers, body)

    @pl.when(hub)
    def _():
        to_peers(barrier)

    tall, wide = spread.shape
    row = lax.broadcasted_iota(jnp.int32, (count, wide), 0)
    col = lax.broadcasted_iota(jnp.int32, (count, wide), 1)
    repeat = jnp.where(col // GROUP == row, 1.0, 0.0).astype(jnp.bfloat16)
    row = lax.broadcasted_iota(jnp.int32, (GROUP, wide), 0)
    col = lax.broadcasted_iota(jnp.int32, (GROUP, wide), 1)
    same = (row == col % GROUP)[None]
    read.wait()
    whole = weights[...]
    high = whole.astype(jnp.bfloat16)
    rest = (whole - high.astype(jnp.float32)).astype(jnp.bfloat16)
    both = jnp.concatenate([high, rest], axis=0)
    full = jnp.dot(both, repeat, preferred_element_type=jnp.float32)
    full = jnp.where(same, full[:, None, :], 0.0)
    spread[...] = full.reshape(tall, wide).astype(jnp.bfloat16)
    squares[...] = jnp.zeros_like(squares)

    def place(layer, way, k):
        return jnp.where(jnp.where(layer < n // 2, 0, 1) == way, k, steps + k)

    def copies(way, k, peer):
        code = pltpu.make_async_remote_copy(
            src_ref=out_code.at[way, k], dst_ref=in_code.at[way, k],
            send_sem=send_sem, recv_sem=recv_sem.at[place(peer, way, k)],
            device_id={"snap": peer}, device_id_type=MESH,
        )
        scale = pltpu.make_async_remote_copy(
            src_ref=out_scale.at[way, k], dst_ref=in_scale.at[way, k],
            send_sem=send_sem, recv_sem=recv_sem.at[place(peer, way, k)],
            device_id={"snap": peer}, device_id_type=MESH,
        )
        return scale, code

    def launch(way, k, peer):
        for copy in copies(way, k, peer):
            copy.start()

    paired = late > 3 and late % 2 == 0 and n == 4
    def in_pair(k, odd):
        k = k - (steps - late)
        return jnp.logical_and(jnp.logical_and(k >= 0, k < late - 2), lax.rem(k, 2) == odd)

    def launch_paired(way, k, peer):
        if not paired:
            launch(way, k, peer)
            return
        leading = jnp.logical_and(final, in_pair(k, 0))
        closing = jnp.logical_and(final, in_pair(k, 1))

        @pl.when(jnp.logical_not(jnp.logical_or(leading, closing)))
        def _():
            launch(way, k, peer)

        @pl.when(closing)
        def _():
            two = pl.ds(k - 1, 2)
            for out, into in ((out_scale, in_scale), (out_code, in_code)):
                pltpu.make_async_remote_copy(
                    src_ref=out.at[way, two], dst_ref=into.at[way, two],
                    send_sem=send_sem, recv_sem=recv_sem.at[place(peer, way, k - 1)],
                    device_id={"snap": peer}, device_id_type=MESH,
                ).start()

    def pack(way, k, value):
        code, scale = encode(value.reshape(widths * GROUP, keep))
        out_code[way, k] = code
        out_scale[way, k] = scale

    def send(way, k, peer, value):
        pack(way, k, value)
        launch(way, k, peer)

    chunk = widths * GROUP // 2 * keep // LANES + 1

    def await_sizes(chunks, more_lines, semaphore):
        some = sizes.at[pl.ds(0, chunks * chunk + more_lines)]
        pltpu.make_async_copy(some, some, semaphore).wait()

    def arrived(way, k):
        if paired and isinstance(way, int) and way == 1:
            leading = jnp.logical_and(z == n - 2, in_pair(k, 0))
            closing = jnp.logical_and(z == n - 2, in_pair(k, 1))

            @pl.when(leading)
            def _():
                await_sizes(2, 0, recv_sem.at[place(z, way, k)])

            @pl.when(jnp.logical_not(jnp.logical_or(leading, closing)))
            def _():
                await_sizes(1, 0, recv_sem.at[place(z, way, k)])
        else:
            await_sizes(1, 0, recv_sem.at[place(z, way, k)])

        return decode(in_code[way, k], in_scale[way, k]).reshape(widths, GROUP, keep)

    def count_squares(value):
        square = value * value
        squares[...] += sum(square[:, :, c:c + LANES] for c in range(0, keep, LANES))

    half = widths * GROUP

    def multiply(i):
        d, t = own(i)
        load(i).wait()

        @pl.when(i + AHEAD < total)
        def _():
            load(i + AHEAD).start()

        both_parts = jnp.dot(
            spread[...], tiles[i].reshape(count * GROUP, keep), preferred_element_type=jnp.float32
        )
        value = (both_parts[:half] + both_parts[half:]).reshape(widths, GROUP, keep)
        part[d, t] = value
        return d, t, value

    for i in range(1, min(AHEAD, total)):
        load(i).start()

    ends_way = jnp.where(first, 0, 1)
    ends_peer = jnp.where(first, 1, n - 2)
    if late > 0:
        second = lax.rem(me, 2) == 1
        held = steps - jnp.where(
            first, jnp.where(second, HOLD_FIRST[1], HOLD_FIRST[0]), jnp.where(second, HOLD_FINAL[1], HOLD_FINAL[0])
        )
    else:
        held = steps

    behind = jnp.where(lax.rem(me, 2) == 1, jnp.where(first, BEHIND[0], BEHIND[1]), 0)

    @pl.when(end)
    def _():
        @pl.loop(0, total)
        def _(i):
            d, _, value = multiply(i)

            @pl.when(i == 0)
            def _():
                pl.semaphore_wait(barrier, 1 if n > 2 else peers)

            @pl.when(d != z)
            def _():
                pack(ends_way, i, value)

            ready = jnp.where(i == 0, 0, i - behind)

            @pl.when(jnp.logical_and(jnp.logical_or(i == 0, ready > 0), ready < held))
            def _():
                launch_paired(ends_way, ready, ends_peer)

        if n == 2:
            to_peers(known)
            pl.semaphore_wait(known, peers - 1)

    def write(t):
        rows = pl.ds(pl.multiple_of(t * GROUP, GROUP), GROUP)
        return pltpu.make_async_copy(part.at[z, t], averages.at[:, rows, :], write_sem)

    def settle(t, value):
        part[z, t] = value
        write(t).start()

    def both_ways(t, value, second, counted):
        @pl.when(second)
        def _():
            settle(t, value)

            @pl.when(counted)
            def _():
                count_squares(value)

        @pl.when(jnp.logical_not(second))
        def _():
            part[z, t] = value

    up_delay = lag_up * (z - 1)
    down_delay = lag_down * (n - 2 - z)

    def pass_up(up):
        @pl.when(jnp.logical_and(up >= 0, up < (n - z) * groups))
        def _():
            d, t = upwards(up)
            value = part[d, t] + arrived(0, up)

            @pl.when(d == z)
            def _():
                s = turned(z, t, 1)
                second = z * groups + s + down_delay < up + up_delay
                both_ways(t, value, second, jnp.logical_or(z != 1, t < groups - late))

            extra = jnp.logical_and(z == n - 2, up < groups + late) if late > 0 else False

            @pl.when(jnp.logical_or(d != z, extra))
            def _():
                send(0, up, z + 1, value)

    def pass_down(down):
        @pl.when(jnp.logical_and(down >= 0, down < (z + 1) * groups))
        def _():
            d, t = downwards(down)
            value = part[d, t] + arrived(1, down)

            @pl.when(d == z)
            def _():
                s = turned(z, t, n - 2)
                second = (n - 1 - z) * groups + s + up_delay <= down + down_delay
                both_ways(t, value, second, jnp.logical_or(z != n - 2, t < groups - late))

            extra = jnp.logical_and(z == 1, down < groups + late) if late > 0 else False

            @pl.when(jnp.logical_or(d != z, extra))
            def _():
                send(1, down, z - 1, value)

    def pass_on(j):
        pass_up(j - up_delay)
        pass_down(j - down_delay)

    @pl.when(middle)
    def _():
        pl.loop(0, head)(lambda i: multiply(i) and None)
        pl.semaphore_wait(barrier, 2 + peers - 1)
        to_peers(known)

        @pl.loop(0, steps - late)
        def _(j):
            pass_on(j)

            for m in range(more):
                @pl.when(more * j + m + head < total)
                def _(m=m):
                    multiply(more * j + m + head)

            @pl.when(j == 2)
            def _():
                pl.semaphore_wait(known, peers - 1)

                @pl.when(jnp.logical_and(z == n - 2, z > 1))
                def _():
                    pl.semaphore_signal(token_down, inc=1, device_id={"snap": z - 1}, device_id_type=MESH)

                @pl.when(jnp.logical_and(z == 1, z < n - 2))
                def _():
                    pl.semaphore_signal(token_up, inc=1, device_id={"snap": z + 1}, device_id_type=MESH)

            @pl.when(j == 4)
            def _():
                @pl.when(z > 1)
                def _():
                    pl.semaphore_wait(token_up, 1)

                @pl.when(jnp.logical_and(z > 1, z < n - 2))
                def _():
                    pl.semaphore_signal(token_up, inc=1, device_id={"snap": z + 1}, device_id_type=MESH)

                @pl.when(z < n - 2)
                def _():
                    pl.semaphore_wait(token_down, 1)

                @pl.when(jnp.logical_and(z > 1, z < n - 2))
                def _():
                    pl.semaphore_signal(token_down, inc=1, device_id={"snap": z - 1}, device_id_type=MESH)

                @pl.when(z == 1)
                def _():
                    pl.semaphore_signal(complete, inc=1, device_id={"snap": z - 1}, device_id_type=MESH)

                @pl.when(z == n - 2)
                def _():
                    pl.semaphore_signal(complete, inc=1, device_id={"snap": z + 1}, device_id_type=MESH)

    if late > 0:
        @pl.when(z == 1)
        def _():
            pl.loop(steps - late - down_delay, 2 * groups)(pass_down)

        @pl.when(z == n - 2)
        def _():
            pl.loop(steps - late - up_delay, 2 * groups)(pass_up)

    @pl.when(end)
    def _():
        @pl.loop(0, groups + late)
        def _(k):
            t = jnp.where(k < groups, k, 2 * groups - 1 - k)
            d = jnp.where(k < groups, z, ends_peer)
            value = part[d, t] + arrived(1 - ends_way, k)
            count_squares(value)

            @pl.when(k < groups)
            def _():
                settle(t, value)

        if n > 2:
            pl.semaphore_wait(complete, 1)

    sums = jnp.sum(jnp.sum(squares[...], axis=1), axis=1, keepdims=True)
    lanes = norms.shape[1]
    row = lax.broadcasted_iota(jnp.int32, (widths, lanes), 0)
    col = lax.broadcasted_iota(jnp.int32, (widths, lanes), 1)
    line = jnp.sum(jnp.where(row == col, sums, 0.0), axis=0, keepdims=True)

    mine = z * peers + me
    lines[mine] = line

    for p in range(n):
        def body(k, p=p):
            @pl.when(jnp.logical_or(p != z, k != me))
            def _():
                pltpu.make_async_remote_copy(
                    src_ref=lines.at[mine], dst_ref=lines.at[mine], send_sem=send_sem, recv_sem=line_recv,
                    device_id={"snap": p, "param": k}, device_id_type=MESH,
                ).start()

        each(peers, body)

    if late > 0:
        @pl.when(end)
        def _():
            pl.loop(held, steps)(lambda k: launch_paired(ends_way, k, ends_peer))

        @pl.when(z == 1)
        def _():
            pl.loop(steps - late, steps - 1)(pass_up)

        @pl.when(z == n - 2)
        def _():
            pl.loop(steps - late, steps - 1)(pass_down)

    def all_sent(layers):
        for layer in layers:
            @pl.when(z == layer)
            def _(layer=layer):
                extra = late * (layer == n - 2) + late * (layer == 1)
                await_sizes((n - 1) * groups + extra, n * peers - 1, send_sem)

    all_sent(range(1, n - 1))
    await_sizes(0, n * peers - 1, line_recv)
    result[...] = jnp.sqrt(jnp.sum(lines[...], axis=0) / jnp.float32(entries))
    hand = pltpu.make_async_copy(result, norms, coeff_sem)
    hand.start()

    if late > 0:
        @pl.when(z == 1)
        def _():
            pass_up(steps - 1)

        @pl.when(z == n - 2)
        def _():
            pass_down(steps - 1)

    all_sent((0, n - 1))
    pltpu.make_async_copy(averages, averages, write_sem).wait()
    hand.wait()


def hand_out(averages, norms, widths):
    def body(averages, norms, averages_out, norms_out, line, row, sems):
        parts = SPLIT
        size = averages.shape[0] // parts


        for k in range(parts):
            some = pl.ds(k * size, size)
            pltpu.make_async_copy(averages.at[some], averages_out.at[some], sems.at[k]).start()

        row[...] = norms[0, :widths]
        write = pltpu.make_async_copy(row, norms_out, sems.at[parts])
        write.start()
        for k in range(parts):
            some = pl.ds(k * size, size)
            pltpu.make_async_copy(averages.at[some], averages_out.at[some], sems.at[k]).wait()
        write.wait()

    anywhere = pl.BlockSpec(memory_space=pl.ANY)
    return pl.pallas_call(
        body,
        out_shape=(
            jax.ShapeDtypeStruct(averages.shape, jnp.float32),
            jax.ShapeDtypeStruct((widths,), jnp.float32),
        ),
        in_specs=[pl.BlockSpec(memory_space=pltpu.VMEM)] * 2,
        out_specs=(anywhere, anywhere),
        scratch_shapes=[pltpu.VMEM((1, 128), jnp.float32), pltpu.VMEM((widths,), jnp.float32), pltpu.SemaphoreType.DMA((SPLIT + 1,))],
        name="hand_out",
    )(pltpu.with_memory_space_constraint(averages, pltpu.VMEM), pltpu.with_memory_space_constraint(norms, pltpu.VMEM))


def on_device(n, peers, snapshots, coeffs):
    count, height, cols = snapshots.shape
    widths = coeffs.shape[0]
    keep = cols // n
    groups, steps, _, _ = shape_of(n, height)
    total = n * groups
    entries = height * cols * peers
    dma = pltpu.SemaphoreType.DMA
    regular = pltpu.SemaphoreType.REGULAR
    averages, norms = pl.pallas_call(
        functools.partial(kernel, n, peers, entries),
        out_shape=(
            jax.ShapeDtypeStruct((widths, height, keep), jnp.float32),
            jax.ShapeDtypeStruct((1, LANES), jnp.float32),
        ),
        in_specs=[pl.BlockSpec(memory_space=pl.ANY), pl.BlockSpec(memory_space=pl.ANY)],
        out_specs=(pl.BlockSpec(memory_space=pl.ANY), pl.BlockSpec(memory_space=pl.ANY)),
        scratch_shapes=[
            pltpu.VMEM((widths, count), jnp.float32),
            pltpu.VMEM((2 * widths * GROUP, count * GROUP), jnp.bfloat16),
            pltpu.VMEM((total, count, GROUP, keep), jnp.bfloat16),
            pltpu.VMEM((n, groups, widths, GROUP, keep), jnp.float32),
            pltpu.VMEM((2, steps, widths * GROUP, keep), jnp.bfloat16),
            pltpu.VMEM((2, steps, 1, LANES), jnp.float32),
            pltpu.VMEM((2, steps, widths * GROUP, keep), jnp.bfloat16),
            pltpu.VMEM((2, steps, 1, LANES), jnp.float32),
            pltpu.VMEM((widths, GROUP, LANES), jnp.float32),
            pltpu.VMEM((n * peers, 1, LANES), jnp.float32),
            pltpu.VMEM((1, LANES), jnp.float32),
            pltpu.VMEM((2 * steps * (widths * GROUP // 2 * keep // LANES + 1) + n * peers, 1, LANES), jnp.float32),
            dma, dma((AHEAD + 1,)), dma, dma, dma((steps + max(2, n // 2) * groups,)), dma,
            regular, regular, regular, regular,
        ],
        compiler_params=pltpu.CompilerParams(
            collective_id=0, has_side_effects=True, vmem_limit_bytes=48 * 1024 * 1024
        ),
        name="reconstruct",
    )(pltpu.with_memory_space_constraint(coeffs, pltpu.HBM), snapshots)
    return hand_out(averages, norms, widths)


def solution(mesh):
    in_specs = (P("snap", "param", None), P(None, "snap"))
    out_specs = (P(None, "param", "snap"), P())
    body = functools.partial(on_device, mesh.shape["snap"], mesh.shape["param"])
    return jax.shard_map(body, mesh=mesh, in_specs=in_specs, out_specs=out_specs, check_vma=False)
```
